16 devices in a mesh: dp: 4 (over z, y), tp: 4 (over x, core).
Axes of the slice: x: 2, y: 2, z: 2, core: 2. Of those that a mesh axis runs over, the one named last changes fastest.
Arguments:
- x: bfloat16 [512, 2560], P('dp'), parts along dimension 0
- ln_attn_gamma: float32 [2560], replicated
- ln_attn_beta: float32 [2560], replicated
- ln_mlp_gamma: float32 [2560], replicated
- ln_mlp_beta: float32 [2560], replicated
- w_qkv: bfloat16 [2560, 32, 3, 80], P(None, 'tp')
- w_out: bfloat16 [32, 1, 80, 2560], P('tp')
- w_up: bfloat16 [2560, 10240], P(None, 'tp')
- w_down: bfloat16 [10240, 2560], P('tp')
- k_cache: bfloat16 [512, 32, 128, 80], P('dp', 'tp'), parts along dimension 0
- v_cache: bfloat16 [512, 32, 128, 80], P('dp', 'tp'), parts along dimension 0
- positions: int32 [512], P('dp'), parts along dimension 0
Outputs:
- output 1: bfloat16 [512, 2560], P('dp'), parts along dimension 0
- output 2: bfloat16 [512, 32, 128, 80], P('dp', 'tp'), parts along dimension 0
- output 3: bfloat16 [512, 32, 128, 80], P('dp', 'tp'), parts along dimension 0
There are 4 independent parts. The reference program is written for one: setup_inputs(seed, part) draws one part's arguments, and reference() takes and returns one part's arrays. A program takes and returns all parts, laid end to end along the dimension named above; an argument that names none is the same for every part.
All inputs are finite; a program needn't handle non-finite values.
Results may differ from the reference program's by a relative error of at most 0.0101179.
Values are sent between devices in bfloat16 or wider.
A program may use at most 1 GiB of HBM per device.

```python
import math
import jax
import jax.numpy as jnp
from jax import lax

D = 2560
GROUPS = 32
QPG = 1
HEAD = 80
FF = 10240
BATCH = 128
SEQ = 128

QKV_SLOTS = QPG + 2
HALF_HEAD = HEAD // 2
SCORE_SCALE = 1.0 / math.sqrt(HEAD)
LN_EPS = 1e-5
ROPE_BASE = 10000.0
NEG_BIG = -1e30


def setup_inputs(seed: int = 0, part: int = 0) -> dict:
    shared_key, part_base = jax.random.split(jax.random.key(seed))
    shared = jax.random.split(shared_key, 8)
    local = jax.random.split(jax.random.fold_in(part_base, part), 8)
    x = jax.random.normal(local[0], (BATCH, D), jnp.float32).astype(jnp.bfloat16)
    ln_attn_gamma = 1.0 + 0.3 * jax.random.normal(shared[0], (D,), jnp.float32)
    ln_attn_beta = 0.3 * jax.random.normal(shared[1], (D,), jnp.float32)
    ln_mlp_gamma = 1.0 + 0.3 * jax.random.normal(shared[2], (D,), jnp.float32)
    ln_mlp_beta = 0.3 * jax.random.normal(shared[3], (D,), jnp.float32)
    w_qkv = (jax.random.normal(shared[4], (D, GROUPS, QKV_SLOTS, HEAD), jnp.float32) * D ** -0.5).astype(jnp.bfloat16)
    w_out = (jax.random.normal(shared[5], (GROUPS, QPG, HEAD, D), jnp.float32) * (GROUPS * QPG * HEAD) ** -0.5).astype(jnp.bfloat16)
    w_up = (jax.random.normal(shared[6], (D, FF), jnp.float32) * D ** -0.5).astype(jnp.bfloat16)
    w_down = (jax.random.normal(shared[7], (FF, D), jnp.float32) * FF ** -0.5).astype(jnp.bfloat16)
    ramp = (2.0 * jnp.arange(SEQ, dtype=jnp.float32) / SEQ - 1.0)[None, None, :, None]
    k_slope = 1.5 * jax.random.normal(local[1], (BATCH, GROUPS, 1, HEAD), jnp.float32)
    k_cache = (jax.random.normal(local[2], (BATCH, GROUPS, SEQ, HEAD), jnp.float32) + ramp * k_slope).astype(jnp.bfloat16)
    v_level = jax.random.normal(local[3], (BATCH, GROUPS, 1, HEAD), jnp.float32)
    v_slope = jax.random.normal(local[4], (BATCH, GROUPS, 1, HEAD), jnp.float32)
    v_cache = (0.5 * jax.random.normal(local[5], (BATCH, GROUPS, SEQ, HEAD), jnp.float32) + v_level + ramp * v_slope).astype(jnp.bfloat16)
    positions = jax.random.randint(local[6], (BATCH,), SEQ // 4, SEQ, dtype=jnp.int32)
    positions = positions.at[0].set(SEQ - 1).at[1].set(SEQ // 4)
    return {'x': x, 'ln_attn_gamma': ln_attn_gamma, 'ln_attn_beta': ln_attn_beta, 'ln_mlp_gamma': ln_mlp_gamma, 'ln_mlp_beta': ln_mlp_beta, 'w_qkv': w_qkv, 'w_out': w_out, 'w_up': w_up, 'w_down': w_down, 'k_cache': k_cache, 'v_cache': v_cache, 'positions': positions}


def layer_norm(act_rows, ln_gamma, ln_beta):
    rows_f32 = act_rows.astype(jnp.float32)
    row_mean = jnp.mean(rows_f32, axis=-1, keepdims=True)
    centred = rows_f32 - row_mean
    row_var = jnp.mean(centred * centred, axis=-1, keepdims=True)
    return (centred * lax.rsqrt(row_var + LN_EPS) * ln_gamma + ln_beta).astype(jnp.bfloat16)


def apply_rotary(vectors, cos_t, sin_t):
    as_f32 = vectors.astype(jnp.float32)
    lower_half = as_f32[..., :HALF_HEAD]
    upper_half = as_f32[..., HALF_HEAD:]
    return jnp.concatenate([lower_half * cos_t - upper_half * sin_t, upper_half * cos_t + lower_half * sin_t], axis=-1).astype(jnp.bfloat16)


def reference(x, ln_attn_gamma, ln_attn_beta, ln_mlp_gamma, ln_mlp_beta, w_qkv, w_out, w_up, w_down, k_cache, v_cache, positions):
    attn_in = layer_norm(x, ln_attn_gamma, ln_attn_beta)
    mlp_in = layer_norm(x, ln_mlp_gamma, ln_mlp_beta)
    qkv_rows = jnp.dot(attn_in, w_qkv.reshape(D, GROUPS * QKV_SLOTS * HEAD), preferred_element_type=jnp.float32).astype(jnp.bfloat16)
    qkv_rows = qkv_rows.reshape(BATCH, GROUPS, QKV_SLOTS, HEAD)
    inv_freq = ROPE_BASE ** (-2.0 * jnp.arange(HALF_HEAD, dtype=jnp.float32) / HEAD)
    angles = positions.astype(jnp.float32)[:, None] * inv_freq[None, :]
    cos_t = jnp.cos(angles)
    sin_t = jnp.sin(angles)
    queries = apply_rotary(qkv_rows[:, :, :QPG], cos_t[:, None, None, :], sin_t[:, None, None, :])
    new_key = apply_rotary(qkv_rows[:, :, QPG], cos_t[:, None, :], sin_t[:, None, :])
    new_value = qkv_rows[:, :, QPG + 1]
    slot_ids = jnp.arange(SEQ)
    write_mask = (slot_ids[None, :] == positions[:, None])[:, None, :, None]
    keys_all = jnp.where(write_mask, new_key[:, :, None, :], k_cache)
    values_all = jnp.where(write_mask, new_value[:, :, None, :], v_cache)
    valid_mask = slot_ids[None, :] <= positions[:, None]

    def attend_group(operands):
        q_grp, k_grp, v_grp = operands
        scores = jnp.einsum('bqh,bsh->bqs', q_grp.astype(jnp.float32), k_grp.astype(jnp.float32)) * SCORE_SCALE
        scores = jnp.where(valid_mask[:, None, :], scores, NEG_BIG)
        attn_probs = jax.nn.softmax(scores, axis=-1).astype(jnp.bfloat16)
        return jnp.einsum('bqs,bsh->bqh', attn_probs.astype(jnp.float32), v_grp.astype(jnp.float32)).astype(jnp.bfloat16)

    context = lax.map(attend_group, (jnp.moveaxis(queries, 1, 0), jnp.moveaxis(keys_all, 1, 0), jnp.moveaxis(values_all, 1, 0)))
    context = jnp.moveaxis(context, 0, 1).reshape(BATCH, GROUPS * QPG * HEAD)
    attn_out = jnp.dot(context, w_out.reshape(GROUPS * QPG * HEAD, D), preferred_element_type=jnp.float32)
    hidden = jax.nn.gelu(jnp.dot(mlp_in, w_up, preferred_element_type=jnp.float32), approximate=False).astype(jnp.bfloat16)
    mlp_out = jnp.dot(hidden, w_down, preferred_element_type=jnp.float32)
    layer_out = (x.astype(jnp.float32) + attn_out + mlp_out).astype(jnp.bfloat16)
    return (layer_out, keys_all, values_all)
```

```python
import functools
import numpy as np
import jax
import jax.numpy as jnp
from jax import lax
from jax.experimental import pallas as pl
from jax.experimental.pallas import tpu as pltpu
from jax.sharding import PartitionSpec as P

LN_EPS = 1e-5
ROPE_BASE = 10000.0
NEG_BIG = -1e30
MESH = pl.DeviceIdType.MESH

ROWS = 128
D = 2560
GROUPS = 8
HEAD = 80
HALF = 40
KV = GROUPS * HEAD
SEQ = 128
BLK = 8
NBLK = ROWS // BLK
WCOLS = 512
NW = D // WCOLS
WSLOTS = 3
QSLOTS = 4


def main_kernel(pos_smem, pos_row, inv_freq, ga, ba, gm, bm, x_ref, wq_hbm, wo_hbm, wu_hbm, wd_hbm, k_hbm, v_hbm,
                part_ref, ko_hbm, vo_hbm,
                kbuf, vbuf, wqbuf, wbuf, wobuf, ain, min_, q_sc, kt_sc, vt_sc, h_sc, acc, ctx,
                ksem, vsem, kosem, vosem, wqsem, wsem, wosem):
    f32, bf16 = jnp.float32, jnp.bfloat16

    def wq_copy(g):
        return pltpu.make_async_copy(wq_hbm.at[pl.ds(g * 240, 240)], wqbuf.at[g % QSLOTS], wqsem.at[g % QSLOTS])

    def k_copy(i):
        rows = pl.ds(i * BLK, BLK)
        return pltpu.make_async_copy(k_hbm.at[rows], kbuf.at[rows], ksem.at[i])

    def v_copy(i):
        rows = pl.ds(i * BLK, BLK)
        return pltpu.make_async_copy(v_hbm.at[rows], vbuf.at[rows], vsem.at[i])

    def ko_copy(i):
        rows = pl.ds(i * BLK, BLK)
        return pltpu.make_async_copy(kbuf.at[rows], ko_hbm.at[rows], kosem.at[i])

    def vo_copy(i):
        rows = pl.ds(i * BLK, BLK)
        return pltpu.make_async_copy(vbuf.at[rows], vo_hbm.at[rows], vosem.at[i])

    def w_copy(hbm, c, n):
        cols = pl.ds(pl.multiple_of(c * WCOLS, WCOLS), WCOLS)
        slot = lax.rem(n, WSLOTS)
        return pltpu.make_async_copy(hbm.at[:, cols], wbuf.at[slot], wsem.at[slot])

    for g in range(QSLOTS):
        wq_copy(g).start()

    gav, bav, gmv, bmv = ga[...], ba[...], gm[...], bm[...]

    def ln_body(r, _):
        rows = pl.ds(pl.multiple_of(r * 16, 16), 16)
        xf = x_ref[rows, :].astype(f32)
        mean = jnp.mean(xf, axis=-1, keepdims=True)
        cen = xf - mean
        var = jnp.mean(cen * cen, axis=-1, keepdims=True)
        nrm = cen * lax.rsqrt(var + LN_EPS)
        ain[rows, :] = (nrm * gav + bav).astype(bf16)
        min_[rows, :] = (nrm * gmv + bmv).astype(bf16)
        return 0

    lax.fori_loop(0, ROWS // 16, ln_body, 0)

    angles = inv_freq[...] * pos_row[...].astype(f32)
    cos_t = jnp.cos(angles)
    sin_t = jnp.sin(angles)

    def rotate(u):
        lo, hi = u[:HALF], u[HALF:]
        return jnp.concatenate([lo * cos_t - hi * sin_t, hi * cos_t + lo * sin_t], axis=0)

    for g in range(GROUPS):
        wq_copy(g).wait()
        y = lax.dot_general(wqbuf[g % QSLOTS], ain[...], (((1,), (1,)), ((), ())), preferred_element_type=f32)
        if g + QSLOTS < GROUPS:
            wq_copy(g + QSLOTS).start()
        else:
            j = g + QSLOTS - GROUPS
            k_copy(j).start()
            v_copy(j).start()
            if j < WSLOTS:
                w_copy(wu_hbm, j, j).start()
        y = y.astype(bf16).astype(f32)
        feat = slice(g * HEAD, (g + 1) * HEAD)
        q_sc[feat, :] = rotate(y[:HEAD]).astype(bf16).astype(f32)
        kt_sc[feat, :] = rotate(y[HEAD:2 * HEAD]).astype(bf16).astype(f32)
        vt_sc[feat, :] = y[2 * HEAD:]
    pltpu.make_async_copy(wo_hbm, wobuf, wosem).start()
    qrows = ctx
    for c in range(KV // 128):
        qrows[:, c * 128:(c + 1) * 128] = q_sc[c * 128:(c + 1) * 128, :].T

    lane8 = lax.broadcasted_iota(jnp.int32, (8, KV), 1)
    sub8 = lax.broadcasted_iota(jnp.int32, (8, KV), 0)
    own8 = (lane8 >= sub8 * HEAD) & (lane8 < sub8 * HEAD + HEAD)
    s_lane = lax.broadcasted_iota(jnp.int32, (8, SEQ), 1)
    c_lane = lax.broadcasted_iota(jnp.int32, (KV, SEQ), 1)
    sel = (lax.broadcasted_iota(jnp.int32, (BLK, BLK * 8), 1) // 8
           == lax.broadcasted_iota(jnp.int32, (BLK, BLK * 8), 0)).astype(f32).astype(bf16)
    zero8 = jnp.zeros((8, SEQ), f32)

    def attend(i):
        k_copy(i).wait()
        v_copy(i).wait()
        base = pl.multiple_of(i * BLK, BLK)
        for j in range(BLK):
            b = base + j
            t = pos_smem[b]
            shift = lax.rem(t - b + SEQ, SEQ)
            hit = c_lane == t
            kbuf[b] = jnp.where(hit, pltpu.roll(kt_sc[...], shift, 1).astype(bf16), kbuf[b])
            vbuf[b] = jnp.where(hit, pltpu.roll(vt_sc[...], shift, 1).astype(bf16), vbuf[b])
        ko_copy(i).start()
        vo_copy(i).start()
        picked = []
        for j in range(0, BLK, 2):
            b0, b1 = base + j, base + j + 1
            qs = []
            for b in (b0, b1):
                row = jnp.broadcast_to(qrows[pl.ds(b, 1), :], (8, KV))
                qs.append(jnp.where(own8, row, 0.0))
            qbd = jnp.concatenate(qs, axis=0).astype(bf16)
            kk = jnp.concatenate([kbuf[b0], kbuf[b1]], axis=1)
            s2 = jnp.dot(qbd, kk, preferred_element_type=f32)
            ps = []
            for n, b in enumerate((b0, b1)):
                s = s2[n * 8:n * 8 + 8, n * SEQ:(n + 1) * SEQ] * (HEAD ** -0.5)
                s = jnp.where(s_lane <= pos_smem[b], s, NEG_BIG)
                e = jnp.exp(s - jnp.max(s, axis=-1, keepdims=True))
                ps.append(e / jnp.sum(e, axis=-1, keepdims=True))
            pbd = jnp.concatenate([jnp.concatenate([ps[0], zero8], axis=1),
                                   jnp.concatenate([zero8, ps[1]], axis=1)], axis=0).astype(bf16)
            vv = jnp.concatenate([vbuf[b0], vbuf[b1]], axis=1)
            c2 = lax.dot_general(pbd, vv, (((1,), (1,)), ((), ())), preferred_element_type=f32)
            picked.append(jnp.where(own8, c2[:8], 0.0))
            picked.append(jnp.where(own8, c2[8:], 0.0))
        stack = jnp.concatenate(picked, axis=0).astype(bf16)
        ctx[pl.ds(base, BLK), :] = jnp.dot(sel, stack, preferred_element_type=f32)

        @pl.when(i + 4 < NBLK)
        def _():
            k_copy(i + 4).start()
            v_copy(i + 4).start()

    def up_body(c, _):
        w_copy(wu_hbm, c, c).wait()
        y = jnp.dot(min_[...], wbuf[lax.rem(c, WSLOTS)], preferred_element_type=f32)
        cols = pl.ds(pl.multiple_of(c * WCOLS, WCOLS), WCOLS)
        h_sc[:, cols] = (0.5 * y * (1.0 + lax.erf(y * (0.5 ** 0.5)))).astype(bf16)
        n = c + WSLOTS

        @pl.when(n < NW)
        def _():
            w_copy(wu_hbm, n, n).start()

        @pl.when(n >= NW)
        def _():
            w_copy(wd_hbm, n - NW, n).start()
        attend(c)
        return 0

    def down_body(c, _):
        n = c + NW
        w_copy(wd_hbm, c, n).wait()
        cols = pl.ds(pl.multiple_of(c * WCOLS, WCOLS), WCOLS)
        acc[:, cols] = jnp.dot(h_sc[...], wbuf[lax.rem(n, WSLOTS)], preferred_element_type=f32)

        @pl.when(c + WSLOTS < NW)
        def _():
            w_copy(wd_hbm, c + WSLOTS, n + WSLOTS).start()
        attend(n)
        return 0

    def rest_body(i, _):
        attend(i)
        return 0

    lax.fori_loop(0, NW, up_body, 0)
    lax.fori_loop(0, NW, down_body, 0)
    lax.fori_loop(2 * NW, NBLK, rest_body, 0)

    pltpu.make_async_copy(wo_hbm, wobuf, wosem).wait()
    cb = ctx[...].astype(bf16)

    def out_body(c, _):
        cols = pl.ds(pl.multiple_of(c * WCOLS, WCOLS), WCOLS)
        part_ref[:, cols] = (acc[:, cols] + jnp.dot(cb, wobuf[:, cols], preferred_element_type=f32)).astype(bf16)
        return 0

    lax.fori_loop(0, NW, out_body, 0)

    def drain(i, _):
        ko_copy(i).wait()
        vo_copy(i).wait()
        return 0

    lax.fori_loop(0, NBLK, drain, 0)


def reduce_kernel(part, x_ref, out_ref, near, far, mine, fin, peer_half,
                  s1, r1, s2, r2, s3, r3):
    f32, bf16 = jnp.float32, jnp.bfloat16
    me = lax.axis_index('tp')
    core = lax.rem(me, 2)
    near_id = me + 1 - 2 * core
    far_id = lax.rem(me + 2, 4)
    half = ROWS // 2
    barrier = pltpu.get_barrier_semaphore()
    for peer in (near_id, far_id):
        pl.semaphore_signal(barrier, inc=1, device_id={'tp': peer}, device_id_type=MESH)
    pl.semaphore_wait(barrier, 2)
    mine_rows = pl.ds(pl.multiple_of(core * half, half), half)
    near_rows = pl.ds(pl.multiple_of((1 - core) * half, half), half)
    c1 = pltpu.make_async_remote_copy(part.at[near_rows], near, s1, r1, device_id={'tp': near_id}, device_id_type=MESH)
    c1.start()
    c1.wait()
    mine[...] = (part[mine_rows, :].astype(f32) + near[...].astype(f32)).astype(bf16)
    c2 = pltpu.make_async_remote_copy(mine, far, s2, r2, device_id={'tp': far_id}, device_id_type=MESH)
    c2.start()
    c2.wait()
    fin[...] = (mine[...].astype(f32) + far[...].astype(f32) + x_ref[mine_rows, :].astype(f32)).astype(bf16)
    c3 = pltpu.make_async_remote_copy(fin, peer_half, s3, r3, device_id={'tp': near_id}, device_id_type=MESH)
    c3.start()
    out_ref[mine_rows, :] = fin[...]
    c3.wait()
    out_ref[near_rows, :] = peer_half[...]


def solution(mesh):
    row_spec = P('dp', None)
    vec_spec = P(None)
    cache_spec = P('dp', 'tp', None, None)
    inv = np.power(np.float64(ROPE_BASE), -2.0 * np.arange(HALF, dtype=np.float64) / HEAD).astype(np.float32)
    inv_tab = np.broadcast_to(inv[:, None], (HALF, ROWS)).copy()
    bf16, f32 = jnp.bfloat16, jnp.float32
    sds = jax.ShapeDtypeStruct
    anyspec = pl.BlockSpec(memory_space=pl.ANY)
    vspec = pl.BlockSpec(memory_space=pltpu.VMEM)
    sspec = pl.BlockSpec(memory_space=pltpu.SMEM)
    dma = pltpu.SemaphoreType.DMA

    main = pl.pallas_call(
        main_kernel,
        out_shape=(sds((ROWS, D), bf16), sds((ROWS, KV, SEQ), bf16), sds((ROWS, KV, SEQ), bf16)),
        in_specs=[sspec] + [vspec] * 7 + [anyspec] * 6,
        out_specs=(vspec, anyspec, anyspec),
        scratch_shapes=[
            pltpu.VMEM((ROWS, KV, SEQ), bf16), pltpu.VMEM((ROWS, KV, SEQ), bf16),
            pltpu.VMEM((QSLOTS, 240, D), bf16), pltpu.VMEM((WSLOTS, D, WCOLS), bf16), pltpu.VMEM((KV, D), bf16),
            pltpu.VMEM((ROWS, D), bf16), pltpu.VMEM((ROWS, D), bf16),
            pltpu.VMEM((KV, ROWS), f32), pltpu.VMEM((KV, ROWS), f32), pltpu.VMEM((KV, ROWS), f32),
            pltpu.VMEM((ROWS, D), bf16), pltpu.VMEM((ROWS, D), f32), pltpu.VMEM((ROWS, KV), f32),
            dma((NBLK,)), dma((NBLK,)), dma((NBLK,)), dma((NBLK,)), dma((QSLOTS,)), dma((WSLOTS,)), dma,
        ],
        compiler_params=pltpu.CompilerParams(vmem_limit_bytes=67043328),
        name='layer',
    )
    half = ROWS // 2
    reduce = pl.pallas_call(
        reduce_kernel,
        out_shape=sds((ROWS, D), bf16),
        in_specs=[vspec, vspec],
        out_specs=vspec,
        scratch_shapes=[pltpu.VMEM((half, D), bf16)] * 5 + [dma] * 6,
        compiler_params=pltpu.CompilerParams(collective_id=0, has_side_effects=True, vmem_limit_bytes=16 << 20),
        name='exchange',
    )

    def device_step(x, ga, ba, gm, bm, w_qkv, w_out, w_up, w_down, k_cache, v_cache, positions):
        kt = jnp.swapaxes(k_cache, 2, 3).reshape(ROWS, KV, SEQ)
        vt = jnp.swapaxes(v_cache, 2, 3).reshape(ROWS, KV, SEQ)
        wq = jnp.transpose(w_qkv, (1, 2, 3, 0)).reshape(3 * KV, D)
        wo = w_out.reshape(KV, D)
        part, ko, vo = main(positions, positions.reshape(1, ROWS), jnp.asarray(inv_tab),
                            ga.reshape(1, D), ba.reshape(1, D), gm.reshape(1, D), bm.reshape(1, D),
                            x, wq, wo, w_up, w_down, kt, vt)
        out = reduce(part, x)
        back = lambda c: jnp.swapaxes(c.reshape(ROWS, GROUPS, HEAD, SEQ), 2, 3)
        return out, back(ko), back(vo)

    return jax.shard_map(device_step, mesh=mesh, in_specs=(row_spec, vec_spec, vec_spec, vec_spec, vec_spec, P(None, 'tp', None, None), P('tp', None, None, None), P(None, 'tp'), P('tp', None), cache_spec, cache_spec, P('dp')), out_specs=(row_spec, cache_spec, cache_spec), check_vma=False)
```

```python
import functools
import numpy as np
import jax
import jax.numpy as jnp
from jax import lax
from jax.experimental import pallas as pl
from jax.experimental.pallas import tpu as pltpu
from jax.sharding import PartitionSpec as P

LN_EPS = 1e-5
ROPE_BASE = 10000.0
NEG_BIG = -1e30
MESH = pl.DeviceIdType.MESH

ROWS = 128
D = 2560
GROUPS = 8
HEAD = 80
HALF = 40
KV = GROUPS * HEAD
SEQ = 128
BLK = 8
NBLK = ROWS // BLK
WCOLS = 512
NW = D // WCOLS
WSLOTS = 3
QROWS = 240
HALF_ROWS = ROWS // 2
CUTS = (24, 104)


def main_kernel(pos_smem, pos_row, inv_freq, ga, ba, gm, bm, x_hbm, wq_hbm, wo_hbm, wu_hbm, wd_hbm, k_hbm, v_hbm,
                kbuf, vbuf, send_ref, keep_ref, xh_ref,
                x_ref, wqbuf, wbuf, ain, min_, q_sc, kt_sc, vt_sc, acc, ctx,
                ksem, vsem, wqsem, wsem, wosem, xsem):
    f32, bf16 = jnp.float32, jnp.bfloat16
    h_sc = ain

    def wq_copy(g):
        rows = pl.ds(g * QROWS, QROWS)
        return pltpu.make_async_copy(wq_hbm.at[rows], wqbuf.at[rows], wqsem.at[g])

    def wo_copy():
        return pltpu.make_async_copy(wo_hbm, wqbuf.at[pl.ds(0, KV)], wosem)

    def kv_start(i):
        k_copy(i).start()
        v_copy(i).start()

    def k_copy(i):
        rows = pl.ds(i * BLK, BLK)
        return pltpu.make_async_copy(k_hbm.at[rows], kbuf.at[rows], ksem.at[i])

    def v_copy(i):
        rows = pl.ds(i * BLK, BLK)
        return pltpu.make_async_copy(v_hbm.at[rows], vbuf.at[rows], vsem.at[i])

    def w_copy(hbm, c, n):
        cols = pl.ds(pl.multiple_of(c * WCOLS, WCOLS), WCOLS)
        slot = lax.rem(n, WSLOTS)
        return pltpu.make_async_copy(hbm.at[:, cols], wbuf.at[slot], wsem.at[slot])

    x_copy = pltpu.make_async_copy(x_hbm, x_ref, xsem)
    x_copy.start()
    for g in range(GROUPS):
        wq_copy(g).start()
    for j in range(WSLOTS):
        kv_start(j)
        w_copy(wu_hbm, j, j).start()
    kv_start(WSLOTS)
    x_copy.wait()

    gav, bav, gmv, bmv = [r[...].reshape(1, D) for r in (ga, ba, gm, bm)]

    def ln_body(r, _):
        rows = pl.ds(pl.multiple_of(r * 16, 16), 16)
        xf = x_ref[rows, :].astype(f32)
        mean = jnp.mean(xf, axis=-1, keepdims=True)
        cen = xf - mean
        var = jnp.mean(cen * cen, axis=-1, keepdims=True)
        nrm = cen * lax.rsqrt(var + LN_EPS)
        ain[rows, :] = (nrm * gav + bav).astype(bf16)
        min_[rows, :] = (nrm * gmv + bmv).astype(bf16)
        return 0

    lax.fori_loop(0, ROWS // 16, ln_body, 0)

    angles = inv_freq[...] * pos_row[...].astype(f32)
    cos_t = jnp.cos(angles)
    sin_t = jnp.sin(angles)

    def rotate(u):
        lo, hi = u[:HALF], u[HALF:]
        return jnp.concatenate([lo * cos_t - hi * sin_t, hi * cos_t + lo * sin_t], axis=0)

    for g in range(GROUPS):
        wq_copy(g).wait()
        y = lax.dot_general(wqbuf[g * QROWS:(g + 1) * QROWS, :], ain[...], (((1,), (1,)), ((), ())), preferred_element_type=f32)
        y = y.astype(bf16).astype(f32)
        feat = slice(g * HEAD, (g + 1) * HEAD)
        q_sc[feat, :] = rotate(y[:HEAD]).astype(bf16).astype(f32)
        kt_sc[feat, :] = rotate(y[HEAD:2 * HEAD]).astype(bf16).astype(f32)
        vt_sc[feat, :] = y[2 * HEAD:]
    wo_copy().start()
    qrows = ctx
    for c in range(KV // 128):
        qrows[:, c * 128:(c + 1) * 128] = q_sc[c * 128:(c + 1) * 128, :].T

    lane8 = lax.broadcasted_iota(jnp.int32, (8, KV), 1)
    sub8 = lax.broadcasted_iota(jnp.int32, (8, KV), 0)
    own8 = (lane8 >= sub8 * HEAD) & (lane8 < sub8 * HEAD + HEAD)
    s_lane = lax.broadcasted_iota(jnp.int32, (8, SEQ), 1)
    c_lane = lax.broadcasted_iota(jnp.int32, (KV, SEQ), 1)
    sel = (lax.broadcasted_iota(jnp.int32, (BLK, BLK * 8), 1) // 8
           == lax.broadcasted_iota(jnp.int32, (BLK, BLK * 8), 0)).astype(f32).astype(bf16)
    zero8 = jnp.zeros((8, SEQ), f32)

    def attend(i):
        k_copy(i).wait()
        v_copy(i).wait()
        base = pl.multiple_of(i * BLK, BLK)
        for j in range(BLK):
            b = base + j
            t = pos_smem[b]
            shift = lax.rem(t - b + SEQ, SEQ)
            hit = c_lane == t
            kbuf[b] = jnp.where(hit, pltpu.roll(kt_sc[...], shift, 1).astype(bf16), kbuf[b])
            vbuf[b] = jnp.where(hit, pltpu.roll(vt_sc[...], shift, 1).astype(bf16), vbuf[b])
        picked = []
        for j in range(0, BLK, 2):
            b0, b1 = base + j, base + j + 1
            qs = []
            for b in (b0, b1):
                row = jnp.broadcast_to(qrows[pl.ds(b, 1), :], (8, KV))
                qs.append(jnp.where(own8, row, 0.0))
            qbd = jnp.concatenate(qs, axis=0).astype(bf16)
            kk = jnp.concatenate([kbuf[b0], kbuf[b1]], axis=1)
            s2 = jnp.dot(qbd, kk, preferred_element_type=f32)
            ps = []
            for n, b in enumerate((b0, b1)):
                s = s2[n * 8:n * 8 + 8, n * SEQ:(n + 1) * SEQ] * (HEAD ** -0.5)
                s = jnp.where(s_lane <= pos_smem[b], s, NEG_BIG)
                e = jnp.exp(s - jnp.max(s, axis=-1, keepdims=True))
                ps.append(e / jnp.sum(e, axis=-1, keepdims=True))
            pbd = jnp.concatenate([jnp.concatenate([ps[0], zero8], axis=1),
                                   jnp.concatenate([zero8, ps[1]], axis=1)], axis=0).astype(bf16)
            vv = jnp.concatenate([vbuf[b0], vbuf[b1]], axis=1)
            c2 = lax.dot_general(pbd, vv, (((1,), (1,)), ((), ())), preferred_element_type=f32)
            picked.append(jnp.where(own8, c2[:8], 0.0))
            picked.append(jnp.where(own8, c2[8:], 0.0))
        stack = jnp.concatenate(picked, axis=0).astype(bf16)
        ctx[pl.ds(base, BLK), :] = jnp.dot(sel, stack, preferred_element_type=f32)

        @pl.when(i + 4 < NBLK)
        def _():
            kv_start(i + 4)

    def up_body(c, _):
        w_copy(wu_hbm, c, c).wait()
        y = jnp.dot(min_[...], wbuf[lax.rem(c, WSLOTS)], preferred_element_type=f32)
        cols = pl.ds(pl.multiple_of(c * WCOLS, WCOLS), WCOLS)
        h_sc[:, cols] = (0.5 * y * (1.0 + lax.erf(y * (0.5 ** 0.5)))).astype(bf16)
        n = c + WSLOTS

        @pl.when(n < NW)
        def _():
            w_copy(wu_hbm, n, n).start()

        @pl.when(n >= NW)
        def _():
            w_copy(wd_hbm, n - NW, n).start()
        attend(c)
        return 0

    def down_body(c, _):
        n = c + NW
        w_copy(wd_hbm, c, n).wait()
        cols = pl.ds(pl.multiple_of(c * WCOLS, WCOLS), WCOLS)
        acc[:, cols] = jnp.dot(h_sc[...], wbuf[lax.rem(n, WSLOTS)], preferred_element_type=f32)

        @pl.when(c + WSLOTS < NW)
        def _():
            w_copy(wd_hbm, c + WSLOTS, n + WSLOTS).start()
        attend(n)
        return 0

    def rest_body(i, _):
        attend(i)
        return 0

    lax.fori_loop(0, NW, up_body, 0)
    lax.fori_loop(0, NW, down_body, 0)
    lax.fori_loop(2 * NW, NBLK, rest_body, 0)

    wo_copy().wait()
    core = lax.rem(lax.axis_index('tp'), 2)
    mine_rows = pl.ds(pl.multiple_of(core * HALF_ROWS, HALF_ROWS), HALF_ROWS)
    near_rows = pl.ds(pl.multiple_of((1 - core) * HALF_ROWS, HALF_ROWS), HALF_ROWS)

    def out_body(c, _):
        cols = pl.ds(pl.multiple_of(c * WCOLS, WCOLS), WCOLS)
        w = wqbuf[0:KV, cols]
        send_ref[:, cols] = (acc[near_rows, cols] + jnp.dot(ctx[near_rows, :].astype(bf16), w, preferred_element_type=f32)).astype(bf16)
        keep_ref[:, cols] = acc[mine_rows, cols] + jnp.dot(ctx[mine_rows, :].astype(bf16), w, preferred_element_type=f32)
        return 0

    lax.fori_loop(0, NW, out_body, 0)
    xh_ref[...] = x_ref[mine_rows, :]


def add_near(keep, near, mine):
    mine[...] = (keep[...] + near[...].astype(jnp.float32)).astype(jnp.bfloat16)


def add_far(mine, far, xh, fin):
    f32 = jnp.float32
    fin[...] = (mine[...].astype(f32) + far[...].astype(f32) + xh[...].astype(f32)).astype(jnp.bfloat16)


def assemble(fin, other, out_hbm, sem):
    core = lax.rem(lax.axis_index('tp'), 2)
    copies = []
    for n, (src, place) in enumerate(((fin, core), (other, 1 - core))):
        rows = pl.ds(pl.multiple_of(place * HALF_ROWS, HALF_ROWS), HALF_ROWS)
        copies.append(pltpu.make_async_copy(src, out_hbm.at[rows], sem.at[n]))
    for c in copies:
        c.start()
    for c in copies:
        c.wait()


def write_rows(first, last, kbuf, vbuf, ko_hbm, vo_hbm, sem):
    copies = []
    for n, (src, dst) in enumerate(((kbuf, ko_hbm), (vbuf, vo_hbm))):
        for r in range(first, last, BLK):
            rows = pl.ds(r, BLK)
            copies.append(pltpu.make_async_copy(src.at[rows], dst.at[rows], sem.at[n]))
    for c in copies:
        c.start()
    for c in copies:
        c.wait()


def first_writer(first, last, kbuf, vbuf, ko_hbm, vo_hbm, kout, vout, sem):
    write_rows(first, last, kbuf, vbuf, ko_hbm, vo_hbm, sem)


def next_writer(first, last, kbuf, vbuf, ko_in, vo_in, ko_hbm, vo_hbm, kout, vout, sem):
    write_rows(first, last, kbuf, vbuf, ko_hbm, vo_hbm, sem)


def solution(mesh):
    row_spec = P('dp', None)
    vec_spec = P(None)
    cache_spec = P('dp', 'tp', None, None)
    inv = np.power(np.float64(ROPE_BASE), -2.0 * np.arange(HALF, dtype=np.float64) / HEAD).astype(np.float32)
    inv_tab = np.broadcast_to(inv[:, None], (HALF, ROWS)).copy()
    bf16, f32 = jnp.bfloat16, jnp.float32
    sds = jax.ShapeDtypeStruct
    anyspec = pl.BlockSpec(memory_space=pl.ANY)
    vspec = pl.BlockSpec(memory_space=pltpu.VMEM)
    sspec = pl.BlockSpec(memory_space=pltpu.SMEM)
    dma = pltpu.SemaphoreType.DMA

    cache = (ROWS, KV, SEQ)
    main = pl.pallas_call(
        main_kernel,
        out_shape=(pltpu.VMEM(cache, bf16), pltpu.VMEM(cache, bf16),
                   pltpu.VMEM((HALF_ROWS, D), bf16), pltpu.VMEM((HALF_ROWS, D), f32), pltpu.VMEM((HALF_ROWS, D), bf16)),
        in_specs=[sspec] + [vspec] * 6 + [anyspec] * 7,
        out_specs=(vspec,) * 5,
        scratch_shapes=[
            pltpu.VMEM((ROWS, D), bf16),
            pltpu.VMEM((3 * KV, D), bf16), pltpu.VMEM((WSLOTS, D, WCOLS), bf16),
            pltpu.VMEM((ROWS, D), bf16), pltpu.VMEM((ROWS, D), bf16),
            pltpu.VMEM((KV, ROWS), f32), pltpu.VMEM((KV, ROWS), f32), pltpu.VMEM((KV, ROWS), f32),
            pltpu.VMEM((ROWS, D), f32), pltpu.VMEM((ROWS, KV), f32),
            dma((NBLK,)), dma((NBLK,)), dma((GROUPS,)), dma((WSLOTS,)), dma, dma,
        ],
        compiler_params=pltpu.CompilerParams(vmem_limit_bytes=22 << 20),
        cost_estimate=pl.CostEstimate(flops=5 * 10**9, bytes_accessed=8 * 10**7, transcendentals=0),
        name='layer',
    )

    def writer(first, last, kbuf, vbuf, olds):
        est = pl.CostEstimate(flops=(last - first) * 10**8, bytes_accessed=(last - first) * 4 * KV * SEQ, transcendentals=0)
        aliases = {0: 2, 1: 3}
        if olds:
            aliases.update({2: 0, 3: 1})
        return pl.pallas_call(
            functools.partial(next_writer if olds else first_writer, first, last),
            out_shape=(sds(cache, bf16), sds(cache, bf16), pltpu.VMEM(cache, bf16), pltpu.VMEM(cache, bf16)),
            in_specs=[vspec, vspec] + [anyspec] * len(olds),
            out_specs=(anyspec, anyspec, vspec, vspec),
            scratch_shapes=[dma((2,))],
            input_output_aliases=aliases,
            compiler_params=pltpu.CompilerParams(vmem_limit_bytes=22 << 20),
            cost_estimate=est,
            name='write%d' % first,
        )(kbuf, vbuf, *olds)

    def small(kernel, name):
        return pl.pallas_call(
            kernel, out_shape=pltpu.VMEM((HALF_ROWS, D), bf16), out_specs=vspec,
            compiler_params=pltpu.CompilerParams(vmem_limit_bytes=1 << 20), name=name)

    near_pairs = [(0, 1), (1, 0), (2, 3), (3, 2)]
    far_pairs = [(0, 2), (2, 0), (1, 3), (3, 1)]

    def device_step(x, ga, ba, gm, bm, w_qkv, w_out, w_up, w_down, k_cache, v_cache, positions):
        kt = jnp.swapaxes(k_cache, 2, 3).reshape(ROWS, KV, SEQ)
        vt = jnp.swapaxes(v_cache, 2, 3).reshape(ROWS, KV, SEQ)
        wq = jnp.transpose(w_qkv, (1, 2, 3, 0)).reshape(3 * KV, D)
        wo = w_out.reshape(KV, D)
        kbuf, vbuf, send, keep, xh = main(positions, positions.reshape(1, ROWS), jnp.asarray(inv_tab), ga, ba, gm, bm,
                                          x, wq, wo, w_up, w_down, kt, vt)
        near = lax.ppermute(send, 'tp', near_pairs)
        ko, vo, kbuf, vbuf = writer(0, CUTS[0], kbuf, vbuf, ())
        mine = small(add_near, 'add_near')(keep, near)
        mine, ko, vo = lax.optimization_barrier((mine, ko, vo))
        far = lax.ppermute(mine, 'tp', far_pairs)
        ko, vo, kbuf, vbuf = writer(CUTS[0], CUTS[1], kbuf, vbuf, (ko, vo))
        fin = small(add_far, 'add_far')(mine, far, xh)
        fin, ko, vo = lax.optimization_barrier((fin, ko, vo))
        other = lax.ppermute(fin, 'tp', near_pairs)
        ko, vo, kbuf, vbuf = writer(CUTS[1], ROWS, kbuf, vbuf, (ko, vo))
        out = pl.pallas_call(
            assemble, out_shape=sds((ROWS, D), bf16), in_specs=[vspec] * 2, out_specs=anyspec,
            scratch_shapes=[dma((2,))], compiler_params=pltpu.CompilerParams(vmem_limit_bytes=1 << 20), name='assemble',
        )(fin, other)
        back = lambda c: jnp.swapaxes(c.reshape(ROWS, GROUPS, HEAD, SEQ), 2, 3)
        return out, back(ko), back(vo)

    return jax.shard_map(device_step, mesh=mesh, in_specs=(row_spec, vec_spec, vec_spec, vec_spec, vec_spec, P(None, 'tp', None, None), P('tp', None, None, None), P(None, 'tp'), P('tp', None), cache_spec, cache_spec, P('dp')), out_specs=(row_spec, cache_spec, cache_spec), check_vma=False)
```

```python
import functools
import numpy as np
import jax
import jax.numpy as jnp
from jax import lax
from jax.experimental import pallas as pl
from jax.experimental.pallas import tpu as pltpu
from jax.sharding import PartitionSpec as P

LN_EPS = 1e-5
ROPE_BASE = 10000.0
NEG_BIG = -1e30
MESH = pl.DeviceIdType.MESH

ROWS = 128
D = 2560
GROUPS = 8
HEAD = 80
HALF = 40
KV = GROUPS * HEAD
SEQ = 128
BLK = 8
NBLK = ROWS // BLK
WCOLS = 512
NW = D // WCOLS
WSLOTS = 3
QROWS = 960
AHEAD = NBLK - 2 * NW
OCOLS = 1280
HALF_ROWS = ROWS // 2
CUTS = (24, 104)
LIMIT = 23200 << 10


def main_kernel(pos_smem, pos_row, inv_freq, ga, ba, gm, bm, x_hbm, wq_hbm, wo_hbm, wu_hbm, wd_hbm, k_hbm, v_hbm,
                kbuf, vbuf, send_ref, keep_ref, xh_ref,
                x_ref, wqbuf, wbuf, ain, qrows, kt_sc, vt_sc, acc, ctx, s_sc, p_sc,
                ksem, vsem, wqsem, wsem, wosem, xsem, xhsem):
    f32, bf16 = jnp.float32, jnp.bfloat16
    h_sc, min_ = ain, x_ref

    def wq_copy(n):
        rows = pl.ds(n * QROWS, QROWS)
        return pltpu.make_async_copy(wq_hbm.at[rows], wqbuf.at[rows], wqsem.at[n])

    def wo_copy():
        return pltpu.make_async_copy(wo_hbm, wqbuf.at[pl.ds(0, KV)], wosem)

    def k_copy(i):
        rows = pl.ds(i * BLK, BLK)
        return pltpu.make_async_copy(k_hbm.at[rows], kbuf.at[rows], ksem.at[i])

    def v_copy(i):
        rows = pl.ds(i * BLK, BLK)
        return pltpu.make_async_copy(v_hbm.at[rows], vbuf.at[rows], vsem.at[i])

    def kv_start(i):
        k_copy(i).start()
        v_copy(i).start()

    def w_copy(hbm, c, n):
        cols = pl.ds(pl.multiple_of(c * WCOLS, WCOLS), WCOLS)
        slot = lax.rem(n, WSLOTS)
        return pltpu.make_async_copy(hbm.at[:, cols], wbuf.at[slot], wsem.at[slot])

    x_copy = pltpu.make_async_copy(x_hbm, x_ref, xsem)
    x_copy.start()
    wq_copy(0).start()
    x_copy.wait()
    wq_copy(1).start()
    core = lax.rem(lax.axis_index('tp'), 2)
    mine_rows = pl.ds(pl.multiple_of(core * HALF_ROWS, HALF_ROWS), HALF_ROWS)
    xh_copy = pltpu.make_async_copy(x_hbm.at[mine_rows], xh_ref, xhsem)
    xh_copy.start()
    kv_start(0)

    gav, bav, gmv, bmv = [r[...].reshape(1, D) for r in (ga, ba, gm, bm)]
    for r in range(0, ROWS, 16):
        rows = slice(r, r + 16)
        xf = x_ref[rows, :].astype(f32)
        mean = jnp.mean(xf, axis=-1, keepdims=True)
        cen = xf - mean
        var = jnp.mean(cen * cen, axis=-1, keepdims=True)
        nrm = cen * lax.rsqrt(var + LN_EPS)
        ain[rows, :] = (nrm * gav + bav).astype(bf16)
        min_[rows, :] = (nrm * gmv + bmv).astype(bf16)

    angles = inv_freq[...] * pos_row[...].astype(f32)
    cos_t = jnp.cos(angles)
    sin_t = jnp.sin(angles)

    def rotate(u):
        lo, hi = u[:HALF], u[HALF:]
        return jnp.concatenate([lo * cos_t - hi * sin_t, hi * cos_t + lo * sin_t], axis=0).astype(bf16)

    queries = []
    for n in range(3 * KV // QROWS):
        wq_copy(n).wait()
        w_copy(wu_hbm, n, n).start()
        kv_start(n + 1)
        y = lax.dot_general(wqbuf[n * QROWS:(n + 1) * QROWS, :], ain[...], (((1,), (1,)), ((), ())), preferred_element_type=f32)
        y = y.astype(bf16).astype(f32)
        for m in range(QROWS // (3 * HEAD)):
            g = n * (QROWS // (3 * HEAD)) + m
            yg = y[m * 3 * HEAD:(m + 1) * 3 * HEAD]
            feat = slice(g * HEAD, (g + 1) * HEAD)
            queries.append(rotate(yg[:HEAD]).astype(f32))
            kt_sc[feat, :] = rotate(yg[HEAD:2 * HEAD])
            vt_sc[feat, :] = yg[2 * HEAD:].astype(bf16)
    wo_copy().start()
    w_copy(wu_hbm, 2, 2).start()
    for i in range(3, AHEAD):
        kv_start(i)
    qall = jnp.concatenate(queries, axis=0)
    for c in range(KV // 128):
        qrows[:, c * 128:(c + 1) * 128] = qall[c * 128:(c + 1) * 128, :].T

    lane8 = lax.broadcasted_iota(jnp.int32, (8, KV), 1)
    sub8 = lax.broadcasted_iota(jnp.int32, (8, KV), 0)
    own8 = (lane8 >= sub8 * HEAD) & (lane8 < sub8 * HEAD + HEAD)
    s_lane = lax.broadcasted_iota(jnp.int32, (8, SEQ), 1)
    c_lane = lax.broadcasted_iota(jnp.int16, (KV, SEQ), 1)
    top16 = lax.broadcasted_iota(jnp.int32, (16, SEQ), 0) < 8
    sel = (lax.broadcasted_iota(jnp.int32, (BLK, BLK * 8), 1) // 8
           == lax.broadcasted_iota(jnp.int32, (BLK, BLK * 8), 0)).astype(f32).astype(bf16)

    def arrive(i):
        k_copy(i).wait()
        v_copy(i).wait()

    def scores(i):
        base = pl.multiple_of(i * BLK, BLK)
        for j in range(0, BLK, 2):
            qs, ks = [], []
            for b in (base + j, base + j + 1):
                t = pos_smem[b]
                shift = lax.rem(t - b + SEQ, SEQ)
                hit = c_lane == t.astype(jnp.int16)
                kn = jnp.where(hit, pltpu.roll(kt_sc[...], shift, 1), kbuf[b])
                kbuf[b] = kn
                ks.append(kn)
                vbuf[b] = jnp.where(hit, pltpu.roll(vt_sc[...], shift, 1), vbuf[b])
                row = jnp.broadcast_to(qrows[pl.ds(b, 1), :], (8, KV))
                qs.append(jnp.where(own8, row, 0.0))
            s2 = jnp.dot(jnp.concatenate(qs, axis=0).astype(bf16), jnp.concatenate(ks, axis=1), preferred_element_type=f32)
            s_sc[j * 8:j * 8 + 8, :] = s2[:8, :SEQ]
            s_sc[j * 8 + 8:j * 8 + 16, :] = s2[8:, SEQ:]

    def soften(i):
        for j in range(BLK):
            s = s_sc[j * 8:j * 8 + 8, :] * (HEAD ** -0.5)
            s = jnp.where(s_lane <= pos_smem[i * BLK + j], s, NEG_BIG)
            e = jnp.exp(s - jnp.max(s, axis=-1, keepdims=True))
            p_sc[j * 8:j * 8 + 8, :] = e / jnp.sum(e, axis=-1, keepdims=True)

    def mix(i):
        base = pl.multiple_of(i * BLK, BLK)
        picked = []
        for j in range(0, BLK, 2):
            p = p_sc[j * 8:j * 8 + 16, :]
            pbd = jnp.concatenate([jnp.where(top16, p, 0.0), jnp.where(top16, 0.0, p)], axis=1).astype(bf16)
            vv = jnp.concatenate([vbuf[base + j], vbuf[base + j + 1]], axis=1)
            c2 = lax.dot_general(pbd, vv, (((1,), (1,)), ((), ())), preferred_element_type=f32)
            picked.append(jnp.where(own8, c2[:8], 0.0))
            picked.append(jnp.where(own8, c2[8:], 0.0))
        stack = jnp.concatenate(picked, axis=0).astype(bf16)
        ctx[pl.ds(base, BLK), :] = jnp.dot(sel, stack, preferred_element_type=f32)

    def attend(i):
        mix(jnp.maximum(i - 2, 0))
        soften(jnp.maximum(i - 1, 0))
        scores(i)

    def split(y):
        low, high = y[:HALF_ROWS], y[HALF_ROWS:]
        return jnp.where(core == 0, low, high), jnp.where(core == 0, high, low)

    def up_dot(c):
        y = jnp.dot(min_[...], wbuf[lax.rem(c, WSLOTS)], preferred_element_type=f32)
        cols = pl.ds(pl.multiple_of(c * WCOLS, WCOLS), WCOLS)
        h_sc[:, cols] = (0.5 * y * (1.0 + lax.erf(y * (0.5 ** 0.5)))).astype(bf16)

    def down_dot(c, n):
        cols = pl.ds(pl.multiple_of(c * WCOLS, WCOLS), WCOLS)
        mine, near = split(jnp.dot(h_sc[...], wbuf[lax.rem(n, WSLOTS)], preferred_element_type=f32))
        keep_ref[:, cols] = mine
        acc[:, cols] = near

    s_sc[...] = jnp.zeros_like(s_sc)
    p_sc[...] = jnp.zeros_like(p_sc)

    def up_body(next_hbm, back, c, _):
        w_copy(wu_hbm, c, c).wait()
        arrive(c)
        up_dot(c)
        attend(c)
        w_copy(next_hbm, c + WSLOTS - back, c + WSLOTS).start()
        kv_start(c + AHEAD)
        return 0

    def down_body(more, c, _):
        n = c + NW
        w_copy(wd_hbm, c, n).wait()
        arrive(n)
        down_dot(c, n)
        attend(n)
        if more:
            w_copy(wd_hbm, c + WSLOTS, n + WSLOTS).start()
        kv_start(n + AHEAD)
        return 0

    def rest_body(i, _):
        arrive(i)
        attend(i)
        return 0

    lax.fori_loop(0, NW - WSLOTS, functools.partial(up_body, wu_hbm, 0), 0)
    lax.fori_loop(NW - WSLOTS, NW, functools.partial(up_body, wd_hbm, NW), 0)
    lax.fori_loop(0, NW - WSLOTS, functools.partial(down_body, True), 0)
    lax.fori_loop(NW - WSLOTS, NW, functools.partial(down_body, False), 0)
    lax.fori_loop(2 * NW, NBLK, rest_body, 0)
    wo_copy().wait()
    mix(NBLK - 2)
    soften(NBLK - 1)
    mix(NBLK - 1)

    cb = ctx[...].astype(bf16)
    for c in range(0, D, OCOLS):
        cols = slice(c, c + OCOLS)
        mine, near = split(jnp.dot(cb, wqbuf[0:KV, cols], preferred_element_type=f32))
        keep_ref[:, cols] += mine
        send_ref[:, cols] = (acc[:, cols] + near).astype(bf16)
    xh_copy.wait()


def add_near(keep, near, mine):
    mine[...] = (keep[...] + near[...].astype(jnp.float32)).astype(jnp.bfloat16)


def add_far(mine, far, xh, fin):
    f32 = jnp.float32
    fin[...] = (mine[...].astype(f32) + far[...].astype(f32) + xh[...].astype(f32)).astype(jnp.bfloat16)


def assemble(fin, other, out_hbm, sem):
    core = lax.rem(lax.axis_index('tp'), 2)
    copies = []
    for n, (src, place) in enumerate(((fin, core), (other, 1 - core))):
        rows = pl.ds(pl.multiple_of(place * HALF_ROWS, HALF_ROWS), HALF_ROWS)
        copies.append(pltpu.make_async_copy(src, out_hbm.at[rows], sem.at[n]))
    for c in copies:
        c.start()
    for c in copies:
        c.wait()


def write_rows(first, last, kbuf, vbuf, ko_hbm, vo_hbm, sem):
    copies = []
    for n, (src, dst) in enumerate(((kbuf, ko_hbm), (vbuf, vo_hbm))):
        for r in range(first, last, BLK):
            rows = pl.ds(r, BLK)
            copies.append(pltpu.make_async_copy(src.at[rows], dst.at[rows], sem.at[n]))
    for c in copies:
        c.start()
    for c in copies:
        c.wait()


def first_writer(first, last, kbuf, vbuf, ko_hbm, vo_hbm, kout, vout, sem):
    write_rows(first, last, kbuf, vbuf, ko_hbm, vo_hbm, sem)


def next_writer(first, last, kbuf, vbuf, ko_in, vo_in, ko_hbm, vo_hbm, kout, vout, sem):
    write_rows(first, last, kbuf, vbuf, ko_hbm, vo_hbm, sem)


def solution(mesh):
    row_spec = P('dp', None)
    vec_spec = P(None)
    cache_spec = P('dp', 'tp', None, None)
    inv = np.power(np.float64(ROPE_BASE), -2.0 * np.arange(HALF, dtype=np.float64) / HEAD).astype(np.float32)
    inv_tab = np.broadcast_to(inv[:, None], (HALF, ROWS)).copy()
    bf16, f32 = jnp.bfloat16, jnp.float32
    sds = jax.ShapeDtypeStruct
    anyspec = pl.BlockSpec(memory_space=pl.ANY)
    vspec = pl.BlockSpec(memory_space=pltpu.VMEM)
    sspec = pl.BlockSpec(memory_space=pltpu.SMEM)
    dma = pltpu.SemaphoreType.DMA

    cache = (ROWS, KV, SEQ)
    main = pl.pallas_call(
        main_kernel,
        out_shape=(pltpu.VMEM(cache, bf16), pltpu.VMEM(cache, bf16),
                   pltpu.VMEM((HALF_ROWS, D), bf16), pltpu.VMEM((HALF_ROWS, D), f32), pltpu.VMEM((HALF_ROWS, D), bf16)),
        in_specs=[sspec] + [vspec] * 6 + [anyspec] * 7,
        out_specs=(vspec,) * 5,
        scratch_shapes=[
            pltpu.VMEM((ROWS, D), bf16),
            pltpu.VMEM((3 * KV, D), bf16), pltpu.VMEM((WSLOTS, D, WCOLS), bf16),
            pltpu.VMEM((ROWS, D), bf16),
            pltpu.VMEM((ROWS, KV), f32), pltpu.VMEM((KV, ROWS), bf16), pltpu.VMEM((KV, ROWS), bf16),
            pltpu.VMEM((HALF_ROWS, D), f32), pltpu.VMEM((ROWS, KV), f32),
            pltpu.VMEM((BLK * 8, SEQ), f32), pltpu.VMEM((BLK * 8, SEQ), f32),
            dma((NBLK,)), dma((NBLK,)), dma((3 * KV // QROWS,)), dma((WSLOTS,)), dma, dma, dma,
        ],
        compiler_params=pltpu.CompilerParams(vmem_limit_bytes=LIMIT),
        cost_estimate=pl.CostEstimate(flops=5 * 10**9, bytes_accessed=8 * 10**7, transcendentals=0),
        name='layer',
    )

    def writer(first, last, kbuf, vbuf, olds):
        est = pl.CostEstimate(flops=(last - first) * 10**8, bytes_accessed=(last - first) * 4 * KV * SEQ, transcendentals=0)
        aliases = {0: 2, 1: 3}
        if olds:
            aliases.update({2: 0, 3: 1})
        return pl.pallas_call(
            functools.partial(next_writer if olds else first_writer, first, last),
            out_shape=(sds(cache, bf16), sds(cache, bf16), pltpu.VMEM(cache, bf16), pltpu.VMEM(cache, bf16)),
            in_specs=[vspec, vspec] + [anyspec] * len(olds),
            out_specs=(anyspec, anyspec, vspec, vspec),
            scratch_shapes=[dma((2,))],
            input_output_aliases=aliases,
            compiler_params=pltpu.CompilerParams(vmem_limit_bytes=LIMIT),
            cost_estimate=est,
            name='write%d' % first,
        )(kbuf, vbuf, *olds)

    def small(kernel, name):
        return pl.pallas_call(
            kernel, out_shape=pltpu.VMEM((HALF_ROWS, D), bf16), out_specs=vspec,
            compiler_params=pltpu.CompilerParams(vmem_limit_bytes=1 << 20), name=name)

    near_pairs = [(0, 1), (1, 0), (2, 3), (3, 2)]
    far_pairs = [(0, 2), (2, 0), (1, 3), (3, 1)]

    def device_step(x, ga, ba, gm, bm, w_qkv, w_out, w_up, w_down, k_cache, v_cache, positions):
        kt = jnp.swapaxes(k_cache, 2, 3).reshape(ROWS, KV, SEQ)
        vt = jnp.swapaxes(v_cache, 2, 3).reshape(ROWS, KV, SEQ)
        wq = jnp.transpose(w_qkv, (1, 2, 3, 0)).reshape(3 * KV, D)
        wo = w_out.reshape(KV, D)
        kbuf, vbuf, send, keep, xh = main(positions, positions.reshape(1, ROWS), jnp.asarray(inv_tab), ga, ba, gm, bm,
                                          x, wq, wo, w_up, w_down, kt, vt)
        near = lax.ppermute(send, 'tp', near_pairs)
        ko, vo, kbuf, vbuf = writer(0, CUTS[0], kbuf, vbuf, ())
        mine = small(add_near, 'add_near')(keep, near)
        mine, ko, vo = lax.optimization_barrier((mine, ko, vo))
        far = lax.ppermute(mine, 'tp', far_pairs)
        ko, vo, kbuf, vbuf = writer(CUTS[0], CUTS[1], kbuf, vbuf, (ko, vo))
        fin = small(add_far, 'add_far')(mine, far, xh)
        fin, ko, vo = lax.optimization_barrier((fin, ko, vo))
        other = lax.ppermute(fin, 'tp', near_pairs)
        ko, vo, kbuf, vbuf = writer(CUTS[1], ROWS, kbuf, vbuf, (ko, vo))
        out = pl.pallas_call(
            assemble, out_shape=sds((ROWS, D), bf16), in_specs=[vspec] * 2, out_specs=anyspec,
            scratch_shapes=[dma((2,))], compiler_params=pltpu.CompilerParams(vmem_limit_bytes=1 << 20), name='assemble',
        )(fin, other)
        back = lambda c: jnp.swapaxes(c.reshape(ROWS, GROUPS, HEAD, SEQ), 2, 3)
        return out, back(ko), back(vo)

    return jax.shard_map(device_step, mesh=mesh, in_specs=(row_spec, vec_spec, vec_spec, vec_spec, vec_spec, P(None, 'tp', None, None), P('tp', None, None, None), P(None, 'tp'), P('tp', None), cache_spec, cache_spec, P('dp')), out_specs=(row_spec, cache_spec, cache_spec), check_vma=False)
```

```python
import functools
import numpy as np
import jax
import jax.numpy as jnp
from jax import lax
from jax.experimental import pallas as pl
from jax.experimental.pallas import tpu as pltpu
from jax.sharding import PartitionSpec as P

LN_EPS = 1e-5
ROPE_BASE = 10000.0
NEG_BIG = -1e30
MESH = pl.DeviceIdType.MESH

ROWS = 128
D = 2560
GROUPS = 8
HEAD = 80
HALF = 40
KV = GROUPS * HEAD
SEQ = 128
BLK = 8
NBLK = ROWS // BLK
WCOLS = 512
NW = D // WCOLS
WSLOTS = 3
QROWS = 960
AHEAD = NBLK - 2 * NW
OCOLS = 1280
HALF_ROWS = ROWS // 2
CUTS = (32, 40, 120)
LIMIT = 22784 << 10


def main_kernel(pos_hbm, pos_row_hbm, inv_hbm, ga_hbm, ba_hbm, gm_hbm, bm_hbm, x_hbm, wq_hbm, wo_hbm, wu_hbm, wd_hbm, k_hbm, v_hbm,
                ko_hbm, vo_hbm, kbuf, vbuf, send_ref, keep_ref, xh_ref,
                pos_smem, pos_row, inv_freq, ga, ba, gm, bm, x_ref, wqbuf, wbuf, ain, qrows, kt_sc, vt_sc, acc, ctx, s_sc, p_sc,
                ksem, vsem, wqsem, wsem, wosem, xsem, xhsem, smsem, outsem):
    f32, bf16 = jnp.float32, jnp.bfloat16
    h_sc, min_ = ain, x_ref

    def wq_copy(n):
        rows = pl.ds(n * QROWS, QROWS)
        return pltpu.make_async_copy(wq_hbm.at[rows], wqbuf.at[rows], wqsem.at[n])

    def wo_copy():
        return pltpu.make_async_copy(wo_hbm, wqbuf.at[pl.ds(0, KV)], wosem)

    def k_copy(i):
        rows = pl.ds(i * BLK, BLK)
        return pltpu.make_async_copy(k_hbm.at[rows], kbuf.at[rows], ksem.at[i])

    def v_copy(i):
        rows = pl.ds(i * BLK, BLK)
        return pltpu.make_async_copy(v_hbm.at[rows], vbuf.at[rows], vsem.at[i])

    def kv_start(i):
        k_copy(i).start()
        v_copy(i).start()

    def w_copy(hbm, c, n):
        cols = pl.ds(pl.multiple_of(c * WCOLS, WCOLS), WCOLS)
        slot = lax.rem(n, WSLOTS)
        return pltpu.make_async_copy(hbm.at[:, cols], wbuf.at[slot], wsem.at[slot])

    x_copy = pltpu.make_async_copy(x_hbm, x_ref, xsem)
    small = [pltpu.make_async_copy(src, dst, smsem.at[n]) for n, (src, dst) in enumerate((
        (pos_hbm, pos_smem), (pos_row_hbm, pos_row), (inv_hbm, inv_freq),
        (ga_hbm, ga), (ba_hbm, ba), (gm_hbm, gm), (bm_hbm, bm)))]
    x_copy.start()
    for c in small:
        c.start()
    wq_copy(0).start()
    for c in small:
        c.wait()
    x_copy.wait()
    wq_copy(1).start()
    core = lax.rem(lax.axis_index('tp'), 2)
    mine_rows = pl.ds(pl.multiple_of(core * HALF_ROWS, HALF_ROWS), HALF_ROWS)
    xh_copy = pltpu.make_async_copy(x_hbm.at[mine_rows], xh_ref, xhsem)
    xh_copy.start()
    kv_start(0)

    gav, bav, gmv, bmv = [r[...].reshape(1, D) for r in (ga, ba, gm, bm)]
    for r in range(0, ROWS, 16):
        rows = slice(r, r + 16)
        xf = x_ref[rows, :].astype(f32)
        mean = jnp.mean(xf, axis=-1, keepdims=True)
        cen = xf - mean
        var = jnp.mean(cen * cen, axis=-1, keepdims=True)
        nrm = cen * lax.rsqrt(var + LN_EPS)
        ain[rows, :] = (nrm * gav + bav).astype(bf16)
        min_[rows, :] = (nrm * gmv + bmv).astype(bf16)

    angles = inv_freq[...] * pos_row[...].astype(f32)
    cos_t = jnp.cos(angles)
    sin_t = jnp.sin(angles)

    def rotate(u):
        lo, hi = u[:HALF], u[HALF:]
        return jnp.concatenate([lo * cos_t - hi * sin_t, hi * cos_t + lo * sin_t], axis=0).astype(bf16)

    queries = []
    for n in range(3 * KV // QROWS):
        wq_copy(n).wait()
        w_copy(wu_hbm, n, n).start()
        kv_start(n + 1)
        y = jnp.concatenate([
            lax.dot_general(wqbuf[r:r + QROWS // 2, :], ain[...], (((1,), (1,)), ((), ())), preferred_element_type=f32)
            for r in (n * QROWS, n * QROWS + QROWS // 2)], axis=0)
        y = y.astype(bf16).astype(f32)
        for m in range(QROWS // (3 * HEAD)):
            g = n * (QROWS // (3 * HEAD)) + m
            yg = y[m * 3 * HEAD:(m + 1) * 3 * HEAD]
            feat = slice(g * HEAD, (g + 1) * HEAD)
            queries.append(rotate(yg[:HEAD]).astype(f32))
            kt_sc[feat, :] = rotate(yg[HEAD:2 * HEAD])
            vt_sc[feat, :] = yg[2 * HEAD:].astype(bf16)
    wo_copy().start()
    w_copy(wu_hbm, 2, 2).start()
    for i in range(3, AHEAD):
        kv_start(i)
    qall = jnp.concatenate(queries, axis=0)
    for c in range(KV // 128):
        qrows[:, c * 128:(c + 1) * 128] = qall[c * 128:(c + 1) * 128, :].T

    lane8 = lax.broadcasted_iota(jnp.int32, (8, KV), 1)
    sub8 = lax.broadcasted_iota(jnp.int32, (8, KV), 0)
    own8 = (lane8 >= sub8 * HEAD) & (lane8 < sub8 * HEAD + HEAD)
    s_lane = lax.broadcasted_iota(jnp.int32, (8, SEQ), 1)
    c_lane = lax.broadcasted_iota(jnp.int16, (KV, SEQ), 1)
    top16 = lax.broadcasted_iota(jnp.int32, (16, SEQ), 0) < 8
    sel = (lax.broadcasted_iota(jnp.int32, (BLK, BLK * 8), 1) // 8
           == lax.broadcasted_iota(jnp.int32, (BLK, BLK * 8), 0)).astype(f32).astype(bf16)

    def arrive(i):
        k_copy(i).wait()
        v_copy(i).wait()

    def scores(i):
        base = pl.multiple_of(i * BLK, BLK)
        for j in range(0, BLK, 2):
            qs, ks = [], []
            for b in (base + j, base + j + 1):
                t = pos_smem[b]
                shift = lax.rem(t - b + SEQ, SEQ)
                hit = c_lane == t.astype(jnp.int16)
                kn = jnp.where(hit, pltpu.roll(kt_sc[...], shift, 1), kbuf[b])
                kbuf[b] = kn
                ks.append(kn)
                vbuf[b] = jnp.where(hit, pltpu.roll(vt_sc[...], shift, 1), vbuf[b])
                row = jnp.broadcast_to(qrows[pl.ds(b, 1), :], (8, KV))
                qs.append(jnp.where(own8, row, 0.0))
            s2 = jnp.dot(jnp.concatenate(qs, axis=0).astype(bf16), jnp.concatenate(ks, axis=1), preferred_element_type=f32)
            s_sc[j * 8:j * 8 + 8, :] = s2[:8, :SEQ]
            s_sc[j * 8 + 8:j * 8 + 16, :] = s2[8:, SEQ:]

    def soften(i):
        for j in range(BLK):
            s = s_sc[j * 8:j * 8 + 8, :] * (HEAD ** -0.5)
            s = jnp.where(s_lane <= pos_smem[i * BLK + j], s, NEG_BIG)
            e = jnp.exp(s - jnp.max(s, axis=-1, keepdims=True))
            p_sc[j * 8:j * 8 + 8, :] = e / jnp.sum(e, axis=-1, keepdims=True)

    def mix(i):
        base = pl.multiple_of(i * BLK, BLK)
        picked = []
        for j in range(0, BLK, 2):
            p = p_sc[j * 8:j * 8 + 16, :]
            pbd = jnp.concatenate([jnp.where(top16, p, 0.0), jnp.where(top16, 0.0, p)], axis=1).astype(bf16)
            vv = jnp.concatenate([vbuf[base + j], vbuf[base + j + 1]], axis=1)
            c2 = lax.dot_general(pbd, vv, (((1,), (1,)), ((), ())), preferred_element_type=f32)
            picked.append(jnp.where(own8, c2[:8], 0.0))
            picked.append(jnp.where(own8, c2[8:], 0.0))
        stack = jnp.concatenate(picked, axis=0).astype(bf16)
        ctx[pl.ds(base, BLK), :] = jnp.dot(sel, stack, preferred_element_type=f32)

    def attend(i):
        mix(jnp.maximum(i - 2, 0))
        soften(jnp.maximum(i - 1, 0))
        scores(i)

    def split(y):
        low, high = y[:HALF_ROWS], y[HALF_ROWS:]
        return jnp.where(core == 0, low, high), jnp.where(core == 0, high, low)

    def up_dot(c):
        y = jnp.dot(min_[...], wbuf[lax.rem(c, WSLOTS)], preferred_element_type=f32)
        cols = pl.ds(pl.multiple_of(c * WCOLS, WCOLS), WCOLS)
        h_sc[:, cols] = (0.5 * y * (1.0 + lax.erf(y * (0.5 ** 0.5)))).astype(bf16)

    def down_dot(c, n):
        cols = pl.ds(pl.multiple_of(c * WCOLS, WCOLS), WCOLS)
        mine, near = split(jnp.dot(h_sc[...], wbuf[lax.rem(n, WSLOTS)], preferred_element_type=f32))
        keep_ref[:, cols] = mine
        acc[:, cols] = near

    s_sc[...] = jnp.zeros_like(s_sc)
    p_sc[...] = jnp.zeros_like(p_sc)

    def up_body(next_hbm, back, c, _):
        w_copy(wu_hbm, c, c).wait()
        arrive(c)
        up_dot(c)
        attend(c)
        w_copy(next_hbm, c + WSLOTS - back, c + WSLOTS).start()
        kv_start(c + AHEAD)
        return 0

    def down_body(more, c, _):
        n = c + NW
        w_copy(wd_hbm, c, n).wait()
        arrive(n)
        down_dot(c, n)
        attend(n)
        if more:
            w_copy(wd_hbm, c + WSLOTS, n + WSLOTS).start()
        kv_start(n + AHEAD)
        return 0

    def rest_body(i, _):
        arrive(i)
        attend(i)
        return 0

    lax.fori_loop(0, NW - WSLOTS, functools.partial(up_body, wu_hbm, 0), 0)
    lax.fori_loop(NW - WSLOTS, NW, functools.partial(up_body, wd_hbm, NW), 0)
    lax.fori_loop(0, NW - WSLOTS, functools.partial(down_body, True), 0)
    lax.fori_loop(NW - WSLOTS, NW, functools.partial(down_body, False), 0)
    outs = []
    for n, (src, dst) in enumerate(((kbuf, ko_hbm), (vbuf, vo_hbm))):
        for r in range(0, CUTS[0], BLK):
            rows = pl.ds(r, BLK)
            outs.append(pltpu.make_async_copy(src.at[rows], dst.at[rows], outsem.at[n, r // BLK]))
    for c in outs:
        c.start()
    lax.fori_loop(2 * NW, NBLK, rest_body, 0)
    wo_copy().wait()
    mix(NBLK - 2)
    soften(NBLK - 1)
    mix(NBLK - 1)

    cb = ctx[...].astype(bf16)
    for c in range(0, D, OCOLS):
        cols = slice(c, c + OCOLS)
        mine, near = split(jnp.dot(cb, wqbuf[0:KV, cols], preferred_element_type=f32))
        keep_ref[:, cols] += mine
        send_ref[:, cols] = (acc[:, cols] + near).astype(bf16)
    xh_copy.wait()
    for c in outs:
        c.wait()


def add_near(keep, near, mine):
    mine[...] = (keep[...] + near[...].astype(jnp.float32)).astype(jnp.bfloat16)


def add_far(mine, far, xh, fin):
    f32 = jnp.float32
    fin[...] = (mine[...].astype(f32) + far[...].astype(f32) + xh[...].astype(f32)).astype(jnp.bfloat16)


def assemble(fin, other, out_hbm, sem):
    core = lax.rem(lax.axis_index('tp'), 2)
    copies = []
    for n, (src, place) in enumerate(((fin, core), (other, 1 - core))):
        rows = pl.ds(pl.multiple_of(place * HALF_ROWS, HALF_ROWS), HALF_ROWS)
        copies.append(pltpu.make_async_copy(src, out_hbm.at[rows], sem.at[n]))
    for c in copies:
        c.start()
    for c in copies:
        c.wait()


def write_rows(first, last, kbuf, vbuf, ko_hbm, vo_hbm, sem):
    copies = []
    for n, (src, dst) in enumerate(((kbuf, ko_hbm), (vbuf, vo_hbm))):
        for r in range(first, last, BLK):
            rows = pl.ds(r, BLK)
            copies.append(pltpu.make_async_copy(src.at[rows], dst.at[rows], sem.at[n]))
    for c in copies:
        c.start()
    for c in copies:
        c.wait()


def writer_kernel(first, last, carried, ko_in, vo_in, *refs):
    write_rows(first, last, refs[0], refs[1], refs[carried], refs[carried + 1], refs[-1])


def solution(mesh):
    row_spec = P('dp', None)
    vec_spec = P(None)
    cache_spec = P('dp', 'tp', None, None)
    inv = np.power(np.float64(ROPE_BASE), -2.0 * np.arange(HALF, dtype=np.float64) / HEAD).astype(np.float32)
    inv_tab = np.broadcast_to(inv[:, None], (HALF, ROWS)).copy()
    bf16, f32 = jnp.bfloat16, jnp.float32
    sds = jax.ShapeDtypeStruct
    anyspec = pl.BlockSpec(memory_space=pl.ANY)
    vspec = pl.BlockSpec(memory_space=pltpu.VMEM)
    sspec = pl.BlockSpec(memory_space=pltpu.SMEM)
    dma = pltpu.SemaphoreType.DMA

    cache = (ROWS, KV, SEQ)
    main = pl.pallas_call(
        main_kernel,
        out_shape=(sds(cache, bf16), sds(cache, bf16), pltpu.VMEM(cache, bf16), pltpu.VMEM(cache, bf16),
                   pltpu.VMEM((HALF_ROWS, D), bf16), pltpu.VMEM((HALF_ROWS, D), f32), pltpu.VMEM((HALF_ROWS, D), bf16)),
        in_specs=[anyspec] * 14,
        out_specs=(anyspec,) * 2 + (vspec,) * 5,
        scratch_shapes=[
            pltpu.SMEM((ROWS,), jnp.int32), pltpu.VMEM((1, ROWS), jnp.int32), pltpu.VMEM((HALF, ROWS), f32),
            pltpu.VMEM((D,), f32), pltpu.VMEM((D,), f32), pltpu.VMEM((D,), f32), pltpu.VMEM((D,), f32),
            pltpu.VMEM((ROWS, D), bf16),
            pltpu.VMEM((3 * KV, D), bf16), pltpu.VMEM((WSLOTS, D, WCOLS), bf16),
            pltpu.VMEM((ROWS, D), bf16),
            pltpu.VMEM((ROWS, KV), f32), pltpu.VMEM((KV, ROWS), bf16), pltpu.VMEM((KV, ROWS), bf16),
            pltpu.VMEM((HALF_ROWS, D), f32), pltpu.VMEM((ROWS, KV), f32),
            pltpu.VMEM((BLK * 8, SEQ), f32), pltpu.VMEM((BLK * 8, SEQ), f32),
            dma((NBLK,)), dma((NBLK,)), dma((3 * KV // QROWS,)), dma((WSLOTS,)), dma, dma, dma, dma((7,)), dma((2, CUTS[0] // BLK)),
        ],
        compiler_params=pltpu.CompilerParams(vmem_limit_bytes=LIMIT),
        cost_estimate=pl.CostEstimate(flops=5 * 10**9, bytes_accessed=8 * 10**7, transcendentals=0),
        name='layer',
    )

    def writer(first, last, ko, vo, *carry):
        return pl.pallas_call(
            functools.partial(writer_kernel, first, last, len(carry)),
            out_shape=(sds(cache, bf16), sds(cache, bf16)) + tuple(pltpu.VMEM(c.shape, c.dtype) for c in carry),
            in_specs=[anyspec, anyspec] + [vspec] * len(carry),
            out_specs=(anyspec, anyspec) + (vspec,) * len(carry),
            scratch_shapes=[dma((2,))],
            input_output_aliases={n: n for n in range(2 + len(carry))},
            compiler_params=pltpu.CompilerParams(vmem_limit_bytes=LIMIT),
            cost_estimate=pl.CostEstimate(flops=(last - first) * 10**8, bytes_accessed=(last - first) * 4 * KV * SEQ, transcendentals=0),
            name='write%d' % first,
        )(ko, vo, *carry)

    def small(kernel, name):
        return pl.pallas_call(
            kernel, out_shape=pltpu.VMEM((HALF_ROWS, D), bf16), out_specs=vspec,
            compiler_params=pltpu.CompilerParams(vmem_limit_bytes=1 << 20), name=name)

    near_pairs = [(0, 1), (1, 0), (2, 3), (3, 2)]
    far_pairs = [(0, 2), (2, 0), (1, 3), (3, 1)]

    def device_step(x, ga, ba, gm, bm, w_qkv, w_out, w_up, w_down, k_cache, v_cache, positions):
        kt = jnp.swapaxes(k_cache, 2, 3).reshape(ROWS, KV, SEQ)
        vt = jnp.swapaxes(v_cache, 2, 3).reshape(ROWS, KV, SEQ)
        wq = jnp.transpose(w_qkv, (1, 2, 3, 0)).reshape(3 * KV, D)
        wo = w_out.reshape(KV, D)
        ko, vo, kbuf, vbuf, send, keep, xh = main(positions, positions.reshape(1, ROWS), jnp.asarray(inv_tab), ga, ba, gm, bm,
                                          x, wq, wo, w_up, w_down, kt, vt)
        near = lax.ppermute(send, 'tp', near_pairs)
        ko, vo, kbuf, vbuf, keep, xh = writer(CUTS[0], CUTS[1], ko, vo, kbuf, vbuf, keep, xh)
        mine = small(add_near, 'add_near')(keep, near)
        mine, ko, vo = lax.optimization_barrier((mine, ko, vo))
        far = lax.ppermute(mine, 'tp', far_pairs)
        ko, vo, kbuf, vbuf, xh = writer(CUTS[1], CUTS[2], ko, vo, kbuf, vbuf, xh)
        fin = small(add_far, 'add_far')(mine, far, xh)
        fin, ko, vo = lax.optimization_barrier((fin, ko, vo))
        other = lax.ppermute(fin, 'tp', near_pairs)
        ko, vo, kbuf, vbuf = writer(CUTS[2], ROWS, ko, vo, kbuf, vbuf)
        out = pl.pallas_call(
            assemble, out_shape=sds((ROWS, D), bf16), in_specs=[vspec] * 2, out_specs=anyspec,
            scratch_shapes=[dma((2,))], compiler_params=pltpu.CompilerParams(vmem_limit_bytes=1 << 20), name='assemble',
        )(fin, other)
        back = lambda c: jnp.swapaxes(c.reshape(ROWS, GROUPS, HEAD, SEQ), 2, 3)
        return out, back(ko), back(vo)

    return jax.shard_map(device_step, mesh=mesh, in_specs=(row_spec, vec_spec, vec_spec, vec_spec, vec_spec, P(None, 'tp', None, None), P('tp', None, None, None), P(None, 'tp'), P('tp', None), cache_spec, cache_spec, P('dp')), out_specs=(row_spec, cache_spec, cache_spec), check_vma=False)
```

```python
import functools
import numpy as np
import jax
import jax.numpy as jnp
from jax import lax
from jax.experimental import pallas as pl
from jax.experimental.pallas import tpu as pltpu
from jax.sharding import PartitionSpec as P

LN_EPS = 1e-5
ROPE_BASE = 10000.0
NEG_BIG = -1e30
MESH = pl.DeviceIdType.MESH

ROWS = 128
D = 2560
GROUPS = 8
HEAD = 80
HALF = 40
KV = GROUPS * HEAD
SEQ = 128
BLK = 8
NBLK = ROWS // BLK
WCOLS = 512
NW = D // WCOLS
WSLOTS = 3
QROWS = 960
AHEAD = 3
OCOLS = 1280
HALF_ROWS = ROWS // 2
CUTS = (32, 40, 120)
LIMIT = 22784 << 10


def main_kernel(pos_hbm, pos_row_hbm, inv_hbm, ga_hbm, ba_hbm, gm_hbm, bm_hbm, x_hbm, wq_hbm, wo_hbm, wu_hbm, wd_hbm, k_hbm, v_hbm,
                ko_hbm, vo_hbm, kbuf, vbuf, send_ref, keep_ref, xh_ref,
                pos_smem, pos_row, inv_freq, ga, ba, gm, bm, x_ref, wqbuf, wbuf, ain, qrows, kt_sc, vt_sc, acc, ctx, s_sc, p_sc,
                ksem, vsem, wqsem, wsem, wosem, xsem, xhsem, smsem, outsem):
    f32, bf16 = jnp.float32, jnp.bfloat16
    h_sc, min_ = ain, x_ref

    def wq_copy(n):
        rows = pl.ds(n * QROWS, QROWS)
        return pltpu.make_async_copy(wq_hbm.at[rows], wqbuf.at[rows], wqsem.at[n])

    def wo_copy():
        return pltpu.make_async_copy(wo_hbm, wqbuf.at[pl.ds(0, KV)], wosem)

    def k_copy(i):
        rows = pl.ds(i * BLK, BLK)
        return pltpu.make_async_copy(k_hbm.at[rows], kbuf.at[rows], ksem.at[i])

    def v_copy(i):
        rows = pl.ds(i * BLK, BLK)
        return pltpu.make_async_copy(v_hbm.at[rows], vbuf.at[rows], vsem.at[i])

    def kv_start(i):
        k_copy(i).start()
        v_copy(i).start()

    def w_copy(hbm, c, n):
        cols = pl.ds(pl.multiple_of(c * WCOLS, WCOLS), WCOLS)
        slot = lax.rem(n, WSLOTS)
        return pltpu.make_async_copy(hbm.at[:, cols], wbuf.at[slot], wsem.at[slot])

    x_copy = pltpu.make_async_copy(x_hbm, x_ref, xsem)
    small = [pltpu.make_async_copy(src, dst, smsem.at[n]) for n, (src, dst) in enumerate((
        (pos_hbm, pos_smem), (pos_row_hbm, pos_row), (inv_hbm, inv_freq),
        (ga_hbm, ga), (ba_hbm, ba), (gm_hbm, gm), (bm_hbm, bm)))]
    x_copy.start()
    for c in small:
        c.start()
    wq_copy(0).start()
    for c in small:
        c.wait()
    x_copy.wait()
    wq_copy(1).start()
    core = lax.rem(lax.axis_index('tp'), 2)
    mine_rows = pl.ds(pl.multiple_of(core * HALF_ROWS, HALF_ROWS), HALF_ROWS)
    xh_copy = pltpu.make_async_copy(x_hbm.at[mine_rows], xh_ref, xhsem)
    xh_copy.start()

    gav, bav, gmv, bmv = [r[...].reshape(1, D) for r in (ga, ba, gm, bm)]
    for r in range(0, ROWS, 16):
        rows = slice(r, r + 16)
        xf = x_ref[rows, :].astype(f32)
        mean = jnp.mean(xf, axis=-1, keepdims=True)
        cen = xf - mean
        var = jnp.mean(cen * cen, axis=-1, keepdims=True)
        nrm = cen * lax.rsqrt(var + LN_EPS)
        ain[rows, :] = (nrm * gav + bav).astype(bf16)
        min_[rows, :] = (nrm * gmv + bmv).astype(bf16)

    angles = inv_freq[...] * pos_row[...].astype(f32)
    cos_t = jnp.cos(angles)
    sin_t = jnp.sin(angles)

    def rotate(u):
        lo, hi = u[:HALF], u[HALF:]
        return jnp.concatenate([lo * cos_t - hi * sin_t, hi * cos_t + lo * sin_t], axis=0).astype(bf16)

    queries = []
    for n in range(3 * KV // QROWS):
        wq_copy(n).wait()
        if n == 0:
            kv_start(0)
            w_copy(wu_hbm, 0, 0).start()
            kv_start(1)
        else:
            w_copy(wu_hbm, 1, 1).start()
            kv_start(2)
            w_copy(wu_hbm, 2, 2).start()
        y = jnp.concatenate([
            lax.dot_general(wqbuf[r:r + QROWS // 2, :], ain[...], (((1,), (1,)), ((), ())), preferred_element_type=f32)
            for r in (n * QROWS, n * QROWS + QROWS // 2)], axis=0)
        y = y.astype(bf16).astype(f32)
        for m in range(QROWS // (3 * HEAD)):
            g = n * (QROWS // (3 * HEAD)) + m
            yg = y[m * 3 * HEAD:(m + 1) * 3 * HEAD]
            feat = slice(g * HEAD, (g + 1) * HEAD)
            queries.append(rotate(yg[:HEAD]).astype(f32))
            kt_sc[feat, :] = rotate(yg[HEAD:2 * HEAD])
            vt_sc[feat, :] = yg[2 * HEAD:].astype(bf16)
    for i in range(3, AHEAD):
        kv_start(i)
    qall = jnp.concatenate(queries, axis=0)
    for c in range(KV // 128):
        qrows[:, c * 128:(c + 1) * 128] = qall[c * 128:(c + 1) * 128, :].T

    lane8 = lax.broadcasted_iota(jnp.int32, (8, KV), 1)
    sub8 = lax.broadcasted_iota(jnp.int32, (8, KV), 0)
    own8 = (lane8 >= sub8 * HEAD) & (lane8 < sub8 * HEAD + HEAD)
    s_lane = lax.broadcasted_iota(jnp.int32, (8, SEQ), 1)
    c_lane = lax.broadcasted_iota(jnp.int16, (KV, SEQ), 1)
    top16 = lax.broadcasted_iota(jnp.int32, (16, SEQ), 0) < 8
    sel = (lax.broadcasted_iota(jnp.int32, (BLK, BLK * 8), 1) // 8
           == lax.broadcasted_iota(jnp.int32, (BLK, BLK * 8), 0)).astype(f32).astype(bf16)

    def arrive(i):
        k_copy(i).wait()
        v_copy(i).wait()

    def scores(i):
        base = pl.multiple_of(i * BLK, BLK)
        for j in range(0, BLK, 2):
            qs, ks = [], []
            for b in (base + j, base + j + 1):
                t = pos_smem[b]
                shift = lax.rem(t - b + SEQ, SEQ)
                hit = c_lane == t.astype(jnp.int16)
                kn = jnp.where(hit, pltpu.roll(kt_sc[...], shift, 1), kbuf[b])
                kbuf[b] = kn
                ks.append(kn)
                vbuf[b] = jnp.where(hit, pltpu.roll(vt_sc[...], shift, 1), vbuf[b])
                row = jnp.broadcast_to(qrows[pl.ds(b, 1), :], (8, KV))
                qs.append(jnp.where(own8, row, 0.0))
            s2 = jnp.dot(jnp.concatenate(qs, axis=0).astype(bf16), jnp.concatenate(ks, axis=1), preferred_element_type=f32)
            s_sc[j * 8:j * 8 + 8, :] = s2[:8, :SEQ]
            s_sc[j * 8 + 8:j * 8 + 16, :] = s2[8:, SEQ:]

    def soften(i):
        for j in range(BLK):
            s = s_sc[j * 8:j * 8 + 8, :] * (HEAD ** -0.5)
            s = jnp.where(s_lane <= pos_smem[i * BLK + j], s, NEG_BIG)
            e = jnp.exp(s - jnp.max(s, axis=-1, keepdims=True))
            p_sc[j * 8:j * 8 + 8, :] = e / jnp.sum(e, axis=-1, keepdims=True)

    def mix(i):
        base = pl.multiple_of(i * BLK, BLK)
        picked = []
        for j in range(0, BLK, 2):
            p = p_sc[j * 8:j * 8 + 16, :]
            pbd = jnp.concatenate([jnp.where(top16, p, 0.0), jnp.where(top16, 0.0, p)], axis=1).astype(bf16)
            vv = jnp.concatenate([vbuf[base + j], vbuf[base + j + 1]], axis=1)
            c2 = lax.dot_general(pbd, vv, (((1,), (1,)), ((), ())), preferred_element_type=f32)
            picked.append(jnp.where(own8, c2[:8], 0.0))
            picked.append(jnp.where(own8, c2[8:], 0.0))
        stack = jnp.concatenate(picked, axis=0).astype(bf16)
        ctx[pl.ds(base, BLK), :] = jnp.dot(sel, stack, preferred_element_type=f32)

    def attend(i):
        mix(jnp.maximum(i - 2, 0))
        soften(jnp.maximum(i - 1, 0))
        scores(i)

    def split(y):
        low, high = y[:HALF_ROWS], y[HALF_ROWS:]
        return jnp.where(core == 0, low, high), jnp.where(core == 0, high, low)

    def up_dot(c):
        y = jnp.dot(min_[...], wbuf[lax.rem(c, WSLOTS)], preferred_element_type=f32)
        cols = pl.ds(pl.multiple_of(c * WCOLS, WCOLS), WCOLS)
        h_sc[:, cols] = (0.5 * y * (1.0 + lax.erf(y * (0.5 ** 0.5)))).astype(bf16)

    def down_dot(c, n):
        cols = pl.ds(pl.multiple_of(c * WCOLS, WCOLS), WCOLS)
        mine, near = split(jnp.dot(h_sc[...], wbuf[lax.rem(n, WSLOTS)], preferred_element_type=f32))
        keep_ref[:, cols] = mine
        acc[:, cols] = near

    s_sc[...] = jnp.zeros_like(s_sc)
    p_sc[...] = jnp.zeros_like(p_sc)

    def up_body(next_hbm, back, c, _):
        w_copy(wu_hbm, c, c).wait()
        arrive(c)
        up_dot(c)
        attend(c)
        w_copy(next_hbm, c + WSLOTS - back, c + WSLOTS).start()
        kv_start(c + AHEAD)
        return 0

    def down_body(more, c, _):
        n = c + NW
        w_copy(wd_hbm, c, n).wait()
        arrive(n)
        down_dot(c, n)
        attend(n)
        if more:
            w_copy(wd_hbm, c + WSLOTS, n + WSLOTS).start()
        kv_start(n + AHEAD)
        return 0

    def rest_body(more, i, _):
        arrive(i)
        attend(i)
        if more:
            kv_start(i + AHEAD)
        return 0

    lax.fori_loop(0, NW - WSLOTS, functools.partial(up_body, wu_hbm, 0), 0)
    lax.fori_loop(NW - WSLOTS, NW, functools.partial(up_body, wd_hbm, NW), 0)
    lax.fori_loop(0, NW - WSLOTS, functools.partial(down_body, True), 0)
    lax.fori_loop(NW - WSLOTS, NW, functools.partial(down_body, False), 0)
    wo_copy().start()
    outs = []
    for n, (src, dst) in enumerate(((kbuf, ko_hbm), (vbuf, vo_hbm))):
        for r in range(0, CUTS[0], BLK):
            rows = pl.ds(r, BLK)
            outs.append(pltpu.make_async_copy(src.at[rows], dst.at[rows], outsem.at[n, r // BLK]))
    for c in outs:
        c.start()
    lax.fori_loop(2 * NW, NBLK - AHEAD, functools.partial(rest_body, True), 0)
    lax.fori_loop(NBLK - AHEAD, NBLK, functools.partial(rest_body, False), 0)
    wo_copy().wait()
    mix(NBLK - 2)
    soften(NBLK - 1)
    mix(NBLK - 1)

    cb = ctx[...].astype(bf16)
    for c in range(0, D, OCOLS):
        cols = slice(c, c + OCOLS)
        mine, near = split(jnp.dot(cb, wqbuf[0:KV, cols], preferred_element_type=f32))
        keep_ref[:, cols] += mine
        send_ref[:, cols] = (acc[:, cols] + near).astype(bf16)
    xh_copy.wait()
    for c in outs:
        c.wait()


def add_near(keep, near, mine):
    mine[...] = (keep[...] + near[...].astype(jnp.float32)).astype(jnp.bfloat16)


def add_far(mine, far, xh, fin):
    f32 = jnp.float32
    fin[...] = (mine[...].astype(f32) + far[...].astype(f32) + xh[...].astype(f32)).astype(jnp.bfloat16)


def assemble(fin, other, out_hbm, sem):
    core = lax.rem(lax.axis_index('tp'), 2)
    copies = []
    for n, (src, place) in enumerate(((fin, core), (other, 1 - core))):
        rows = pl.ds(pl.multiple_of(place * HALF_ROWS, HALF_ROWS), HALF_ROWS)
        copies.append(pltpu.make_async_copy(src, out_hbm.at[rows], sem.at[n]))
    for c in copies:
        c.start()
    for c in copies:
        c.wait()


def write_rows(first, last, kbuf, vbuf, ko_hbm, vo_hbm, sem):
    copies = []
    for n, (src, dst) in enumerate(((kbuf, ko_hbm), (vbuf, vo_hbm))):
        for r in range(first, last, BLK):
            rows = pl.ds(r, BLK)
            copies.append(pltpu.make_async_copy(src.at[rows], dst.at[rows], sem.at[n]))
    for c in copies:
        c.start()
    for c in copies:
        c.wait()


def writer_kernel(first, last, carried, ko_in, vo_in, *refs):
    write_rows(first, last, refs[0], refs[1], refs[carried], refs[carried + 1], refs[-1])


def solution(mesh):
    row_spec = P('dp', None)
    vec_spec = P(None)
    cache_spec = P('dp', 'tp', None, None)
    inv = np.power(np.float64(ROPE_BASE), -2.0 * np.arange(HALF, dtype=np.float64) / HEAD).astype(np.float32)
    inv_tab = np.broadcast_to(inv[:, None], (HALF, ROWS)).copy()
    bf16, f32 = jnp.bfloat16, jnp.float32
    sds = jax.ShapeDtypeStruct
    anyspec = pl.BlockSpec(memory_space=pl.ANY)
    vspec = pl.BlockSpec(memory_space=pltpu.VMEM)
    sspec = pl.BlockSpec(memory_space=pltpu.SMEM)
    dma = pltpu.SemaphoreType.DMA

    cache = (ROWS, KV, SEQ)
    main = pl.pallas_call(
        main_kernel,
        out_shape=(sds(cache, bf16), sds(cache, bf16), pltpu.VMEM(cache, bf16), pltpu.VMEM(cache, bf16),
                   pltpu.VMEM((HALF_ROWS, D), bf16), pltpu.VMEM((HALF_ROWS, D), f32), pltpu.VMEM((HALF_ROWS, D), bf16)),
        in_specs=[anyspec] * 14,
        out_specs=(anyspec,) * 2 + (vspec,) * 5,
        scratch_shapes=[
            pltpu.SMEM((ROWS,), jnp.int32), pltpu.VMEM((1, ROWS), jnp.int32), pltpu.VMEM((HALF, ROWS), f32),
            pltpu.VMEM((D,), f32), pltpu.VMEM((D,), f32), pltpu.VMEM((D,), f32), pltpu.VMEM((D,), f32),
            pltpu.VMEM((ROWS, D), bf16),
            pltpu.VMEM((3 * KV, D), bf16), pltpu.VMEM((WSLOTS, D, WCOLS), bf16),
            pltpu.VMEM((ROWS, D), bf16),
            pltpu.VMEM((ROWS, KV), f32), pltpu.VMEM((KV, ROWS), bf16), pltpu.VMEM((KV, ROWS), bf16),
            pltpu.VMEM((HALF_ROWS, D), f32), pltpu.VMEM((ROWS, KV), f32),
            pltpu.VMEM((BLK * 8, SEQ), f32), pltpu.VMEM((BLK * 8, SEQ), f32),
            dma((NBLK,)), dma((NBLK,)), dma((3 * KV // QROWS,)), dma((WSLOTS,)), dma, dma, dma, dma((7,)), dma((2, CUTS[0] // BLK)),
        ],
        compiler_params=pltpu.CompilerParams(vmem_limit_bytes=LIMIT),
        cost_estimate=pl.CostEstimate(flops=5 * 10**9, bytes_accessed=8 * 10**7, transcendentals=0),
        name='layer',
    )

    def writer(first, last, ko, vo, *carry):
        return pl.pallas_call(
            functools.partial(writer_kernel, first, last, len(carry)),
            out_shape=(sds(cache, bf16), sds(cache, bf16)) + tuple(pltpu.VMEM(c.shape, c.dtype) for c in carry),
            in_specs=[anyspec, anyspec] + [vspec] * len(carry),
            out_specs=(anyspec, anyspec) + (vspec,) * len(carry),
            scratch_shapes=[dma((2,))],
            input_output_aliases={n: n for n in range(2 + len(carry))},
            compiler_params=pltpu.CompilerParams(vmem_limit_bytes=LIMIT),
            cost_estimate=pl.CostEstimate(flops=(last - first) * 10**8, bytes_accessed=(last - first) * 4 * KV * SEQ, transcendentals=0),
            name='write%d' % first,
        )(ko, vo, *carry)

    def small(kernel, name):
        return pl.pallas_call(
            kernel, out_shape=pltpu.VMEM((HALF_ROWS, D), bf16), out_specs=vspec,
            compiler_params=pltpu.CompilerParams(vmem_limit_bytes=1 << 20), name=name)

    near_pairs = [(0, 1), (1, 0), (2, 3), (3, 2)]
    far_pairs = [(0, 2), (2, 0), (1, 3), (3, 1)]

    def device_step(x, ga, ba, gm, bm, w_qkv, w_out, w_up, w_down, k_cache, v_cache, positions):
        kt = jnp.swapaxes(k_cache, 2, 3).reshape(ROWS, KV, SEQ)
        vt = jnp.swapaxes(v_cache, 2, 3).reshape(ROWS, KV, SEQ)
        wq = jnp.transpose(w_qkv, (1, 2, 3, 0)).reshape(3 * KV, D)
        wo = w_out.reshape(KV, D)
        ko, vo, kbuf, vbuf, send, keep, xh = main(positions, positions.reshape(1, ROWS), jnp.asarray(inv_tab), ga, ba, gm, bm,
                                          x, wq, wo, w_up, w_down, kt, vt)
        near = lax.ppermute(send, 'tp', near_pairs)
        ko, vo, kbuf, vbuf, keep, xh = writer(CUTS[0], CUTS[1], ko, vo, kbuf, vbuf, keep, xh)
        mine = small(add_near, 'add_near')(keep, near)
        mine, ko, vo = lax.optimization_barrier((mine, ko, vo))
        far = lax.ppermute(mine, 'tp', far_pairs)
        ko, vo, kbuf, vbuf, xh = writer(CUTS[1], CUTS[2], ko, vo, kbuf, vbuf, xh)
        fin = small(add_far, 'add_far')(mine, far, xh)
        fin, ko, vo = lax.optimization_barrier((fin, ko, vo))
        other = lax.ppermute(fin, 'tp', near_pairs)
        ko, vo, kbuf, vbuf = writer(CUTS[2], ROWS, ko, vo, kbuf, vbuf)
        out = pl.pallas_call(
            assemble, out_shape=sds((ROWS, D), bf16), in_specs=[vspec] * 2, out_specs=anyspec,
            scratch_shapes=[dma((2,))], compiler_params=pltpu.CompilerParams(vmem_limit_bytes=1 << 20), name='assemble',
        )(fin, other)
        back = lambda c: jnp.swapaxes(c.reshape(ROWS, GROUPS, HEAD, SEQ), 2, 3)
        return out, back(ko), back(vo)

    return jax.shard_map(device_step, mesh=mesh, in_specs=(row_spec, vec_spec, vec_spec, vec_spec, vec_spec, P(None, 'tp', None, None), P('tp', None, None, None), P(None, 'tp'), P('tp', None), cache_spec, cache_spec, P('dp')), out_specs=(row_spec, cache_spec, cache_spec), check_vma=False)
```

```python
import functools
import numpy as np
import jax
import jax.numpy as jnp
from jax import lax
from jax.experimental import pallas as pl
from jax.experimental.pallas import tpu as pltpu
from jax.sharding import PartitionSpec as P

LN_EPS = 1e-5
ROPE_BASE = 10000.0
NEG_BIG = -1e30
MESH = pl.DeviceIdType.MESH

ROWS = 128
D = 2560
GROUPS = 8
HEAD = 80
HALF = 40
KV = GROUPS * HEAD
SEQ = 128
BLK = 8
NBLK = ROWS // BLK
WCOLS = 512
NW = D // WCOLS
WSLOTS = 3
QROWS = 960
AHEAD = 4
OCOLS = 1280
OROWS = 8
HALF_ROWS = ROWS // 2
CUTS = (AHEAD * OROWS, 40, 120)
LIMIT = 22784 << 10


def main_kernel(pos_hbm, pos_row_hbm, inv_hbm, ga_hbm, ba_hbm, gm_hbm, bm_hbm, x_hbm, wq_hbm, wo_hbm, wu_hbm, wd_hbm, k_hbm, v_hbm,
                ko_hbm, vo_hbm, kbuf, vbuf, send_ref, keep_ref, xh_ref,
                pos_smem, pos_row, inv_freq, ga, ba, gm, bm, x_ref, wqbuf, wbuf, ain, qrows, kt_sc, vt_sc, acc, ctx, s_sc, p_sc,
                ksem, vsem, wqsem, wsem, wosem, xsem, xhsem, smsem, outsem):
    f32, bf16 = jnp.float32, jnp.bfloat16
    h_sc, min_ = ain, x_ref

    def wq_copy(n):
        rows = pl.ds(n * (QROWS // 2), QROWS // 2)
        return pltpu.make_async_copy(wq_hbm.at[rows], wqbuf.at[rows], wqsem.at[n])

    def wo_copy():
        return pltpu.make_async_copy(wo_hbm, wqbuf.at[pl.ds(0, KV)], wosem)

    def k_copy(i):
        rows = pl.ds(i * BLK, BLK)
        return pltpu.make_async_copy(k_hbm.at[rows], kbuf.at[rows], ksem.at[i])

    def v_copy(i):
        rows = pl.ds(i * BLK, BLK)
        return pltpu.make_async_copy(v_hbm.at[rows], vbuf.at[rows], vsem.at[i])

    def kv_start(i):
        k_copy(i).start()
        v_copy(i).start()

    def w_copy(hbm, c, n):
        cols = pl.ds(pl.multiple_of(c * WCOLS, WCOLS), WCOLS)
        slot = lax.rem(n, WSLOTS)
        return pltpu.make_async_copy(hbm.at[:, cols], wbuf.at[slot], wsem.at[slot])

    x_copy = pltpu.make_async_copy(x_hbm, x_ref, xsem)
    small = [pltpu.make_async_copy(src, dst, smsem.at[n]) for n, (src, dst) in enumerate((
        (pos_hbm, pos_smem), (pos_row_hbm, pos_row), (inv_hbm, inv_freq),
        (ga_hbm, ga), (ba_hbm, ba), (gm_hbm, gm), (bm_hbm, bm)))]
    x_copy.start()
    for c in small:
        c.start()
    wq_copy(0).start()
    for c in small:
        c.wait()
    x_copy.wait()
    for n in range(1, 4):
        wq_copy(n).start()
    core = lax.rem(lax.axis_index('tp'), 2)
    mine_rows = pl.ds(pl.multiple_of(core * HALF_ROWS, HALF_ROWS), HALF_ROWS)
    xh_copy = pltpu.make_async_copy(x_hbm.at[mine_rows], xh_ref, xhsem)
    xh_copy.start()

    gav, bav, gmv, bmv = [r[...].reshape(1, D) for r in (ga, ba, gm, bm)]
    for r in range(0, ROWS, 16):
        rows = slice(r, r + 16)
        xf = x_ref[rows, :].astype(f32)
        mean = jnp.mean(xf, axis=-1, keepdims=True)
        cen = xf - mean
        var = jnp.mean(cen * cen, axis=-1, keepdims=True)
        nrm = cen * lax.rsqrt(var + LN_EPS)
        ain[rows, :] = (nrm * gav + bav).astype(bf16)
        min_[rows, :] = (nrm * gmv + bmv).astype(bf16)

    angles = inv_freq[...] * pos_row[...].astype(f32)
    cos_t = jnp.cos(angles)
    sin_t = jnp.sin(angles)

    def rotate(u):
        lo, hi = u[:HALF], u[HALF:]
        return jnp.concatenate([lo * cos_t - hi * sin_t, hi * cos_t + lo * sin_t], axis=0).astype(bf16)

    queries = []
    for n in range(3 * KV // QROWS):
        wq_copy(2 * n).wait()
        wq_copy(2 * n + 1).wait()
        if n == 0:
            kv_start(0)
            w_copy(wu_hbm, 0, 0).start()
            kv_start(1)
        else:
            w_copy(wu_hbm, 1, 1).start()
            kv_start(2)
            w_copy(wu_hbm, 2, 2).start()
        y = jnp.concatenate([
            lax.dot_general(wqbuf[r:r + QROWS // 2, :], ain[...], (((1,), (1,)), ((), ())), preferred_element_type=f32)
            for r in (n * QROWS, n * QROWS + QROWS // 2)], axis=0)
        y = y.astype(bf16).astype(f32)
        for m in range(QROWS // (3 * HEAD)):
            g = n * (QROWS // (3 * HEAD)) + m
            yg = y[m * 3 * HEAD:(m + 1) * 3 * HEAD]
            feat = slice(g * HEAD, (g + 1) * HEAD)
            queries.append(rotate(yg[:HEAD]).astype(f32))
            kt_sc[feat, :] = rotate(yg[HEAD:2 * HEAD])
            vt_sc[feat, :] = yg[2 * HEAD:].astype(bf16)
    for i in range(3, AHEAD):
        kv_start(i)
    qall = jnp.concatenate(queries, axis=0)
    for c in range(KV // 128):
        qrows[:, c * 128:(c + 1) * 128] = qall[c * 128:(c + 1) * 128, :].T

    lane8 = lax.broadcasted_iota(jnp.int32, (8, KV), 1)
    sub8 = lax.broadcasted_iota(jnp.int32, (8, KV), 0)
    own8 = (lane8 >= sub8 * HEAD) & (lane8 < sub8 * HEAD + HEAD)
    s_lane = lax.broadcasted_iota(jnp.int32, (8, SEQ), 1)
    c_lane = lax.broadcasted_iota(jnp.int16, (KV, SEQ), 1)
    top16 = lax.broadcasted_iota(jnp.int32, (16, SEQ), 0) < 8
    sel = (lax.broadcasted_iota(jnp.int32, (BLK, BLK * 8), 1) // 8
           == lax.broadcasted_iota(jnp.int32, (BLK, BLK * 8), 0)).astype(f32).astype(bf16)

    def arrive(i):
        k_copy(i).wait()
        v_copy(i).wait()

    def scores(i):
        base = pl.multiple_of(i * BLK, BLK)
        for j in range(0, BLK, 2):
            qs, ks = [], []
            for b in (base + j, base + j + 1):
                t = pos_smem[b]
                shift = lax.rem(t - b + SEQ, SEQ)
                hit = c_lane == t.astype(jnp.int16)
                kn = jnp.where(hit, pltpu.roll(kt_sc[...], shift, 1), kbuf[b])
                kbuf[b] = kn
                ks.append(kn)
                vbuf[b] = jnp.where(hit, pltpu.roll(vt_sc[...], shift, 1), vbuf[b])
                row = jnp.broadcast_to(qrows[pl.ds(b, 1), :], (8, KV))
                qs.append(jnp.where(own8, row, 0.0))
            s2 = jnp.dot(jnp.concatenate(qs, axis=0).astype(bf16), jnp.concatenate(ks, axis=1), preferred_element_type=f32)
            s_sc[j * 8:j * 8 + 8, :] = s2[:8, :SEQ]
            s_sc[j * 8 + 8:j * 8 + 16, :] = s2[8:, SEQ:]

    def soften(i):
        for j in range(BLK):
            s = s_sc[j * 8:j * 8 + 8, :] * (HEAD ** -0.5)
            s = jnp.where(s_lane <= pos_smem[i * BLK + j], s, NEG_BIG)
            e = jnp.exp(s - jnp.max(s, axis=-1, keepdims=True))
            p_sc[j * 8:j * 8 + 8, :] = e / jnp.sum(e, axis=-1, keepdims=True)

    def mix(i):
        base = pl.multiple_of(i * BLK, BLK)
        picked = []
        for j in range(0, BLK, 2):
            p = p_sc[j * 8:j * 8 + 16, :]
            pbd = jnp.concatenate([jnp.where(top16, p, 0.0), jnp.where(top16, 0.0, p)], axis=1).astype(bf16)
            vv = jnp.concatenate([vbuf[base + j], vbuf[base + j + 1]], axis=1)
            c2 = lax.dot_general(pbd, vv, (((1,), (1,)), ((), ())), preferred_element_type=f32)
            picked.append(jnp.where(own8, c2[:8], 0.0))
            picked.append(jnp.where(own8, c2[8:], 0.0))
        stack = jnp.concatenate(picked, axis=0).astype(bf16)
        ctx[pl.ds(base, BLK), :] = jnp.dot(sel, stack, preferred_element_type=f32)

    def attend(i):
        mix(jnp.maximum(i - 2, 0))
        soften(jnp.maximum(i - 1, 0))
        scores(i)

    def split(y):
        low, high = y[:HALF_ROWS], y[HALF_ROWS:]
        return jnp.where(core == 0, low, high), jnp.where(core == 0, high, low)

    def up_dot(c):
        y = jnp.dot(min_[...], wbuf[lax.rem(c, WSLOTS)], preferred_element_type=f32)
        cols = pl.ds(pl.multiple_of(c * WCOLS, WCOLS), WCOLS)
        h_sc[:, cols] = (0.5 * y * (1.0 + lax.erf(y * (0.5 ** 0.5)))).astype(bf16)

    def down_dot(c, n):
        cols = pl.ds(pl.multiple_of(c * WCOLS, WCOLS), WCOLS)
        mine, near = split(jnp.dot(h_sc[...], wbuf[lax.rem(n, WSLOTS)], preferred_element_type=f32))
        keep_ref[:, cols] = mine
        acc[:, cols] = near

    def out_copies(j):
        rows = pl.ds(j * OROWS, OROWS)
        return [pltpu.make_async_copy(src.at[rows], dst.at[rows], outsem.at[n, j])
                for n, (src, dst) in enumerate(((kbuf, ko_hbm), (vbuf, vo_hbm)))]

    s_sc[...] = jnp.zeros_like(s_sc)
    p_sc[...] = jnp.zeros_like(p_sc)

    def up_body(next_hbm, back, c, _):
        w_copy(wu_hbm, c, c).wait()
        arrive(c)
        up_dot(c)
        attend(c)
        w_copy(next_hbm, c + WSLOTS - back, c + WSLOTS).start()
        kv_start(c + AHEAD)
        return 0

    def down_body(more, c, _):
        n = c + NW
        w_copy(wd_hbm, c, n).wait()
        arrive(n)
        down_dot(c, n)
        attend(n)
        if more:
            w_copy(wd_hbm, c + WSLOTS, n + WSLOTS).start()
        kv_start(n + AHEAD)
        return 0

    def rest_body(more, i, _):
        arrive(i)
        attend(i)
        if more:
            kv_start(i + AHEAD)
        else:
            for c in out_copies(i - (NBLK - AHEAD)):
                c.start()
        return 0

    lax.fori_loop(0, NW - WSLOTS, functools.partial(up_body, wu_hbm, 0), 0)
    lax.fori_loop(NW - WSLOTS, NW, functools.partial(up_body, wd_hbm, NW), 0)
    lax.fori_loop(0, NW - WSLOTS, functools.partial(down_body, True), 0)
    lax.fori_loop(NW - WSLOTS, NW, functools.partial(down_body, False), 0)
    wo_copy().start()
    lax.fori_loop(2 * NW, NBLK - AHEAD, functools.partial(rest_body, True), 0)
    lax.fori_loop(NBLK - AHEAD, NBLK, functools.partial(rest_body, False), 0)
    wo_copy().wait()
    mix(NBLK - 2)
    soften(NBLK - 1)
    mix(NBLK - 1)

    cb = ctx[...].astype(bf16)
    for c in range(0, D, OCOLS):
        cols = slice(c, c + OCOLS)
        mine, near = split(jnp.dot(cb, wqbuf[0:KV, cols], preferred_element_type=f32))
        keep_ref[:, cols] += mine
        send_ref[:, cols] = (acc[:, cols] + near).astype(bf16)
    xh_copy.wait()
    for j in range(AHEAD):
        for c in out_copies(j):
            c.wait()


def add_near(keep, near, mine):
    mine[...] = (keep[...] + near[...].astype(jnp.float32)).astype(jnp.bfloat16)


def add_far(mine, far, xh, fin):
    f32 = jnp.float32
    fin[...] = (mine[...].astype(f32) + far[...].astype(f32) + xh[...].astype(f32)).astype(jnp.bfloat16)


def assemble(fin, other, out_hbm, sem):
    core = lax.rem(lax.axis_index('tp'), 2)
    copies = []
    for n, (src, place) in enumerate(((fin, core), (other, 1 - core))):
        rows = pl.ds(pl.multiple_of(place * HALF_ROWS, HALF_ROWS), HALF_ROWS)
        copies.append(pltpu.make_async_copy(src, out_hbm.at[rows], sem.at[n]))
    for c in copies:
        c.start()
    for c in copies:
        c.wait()


def write_rows(first, last, kbuf, vbuf, ko_hbm, vo_hbm, sem):
    copies = []
    for n, (src, dst) in enumerate(((kbuf, ko_hbm), (vbuf, vo_hbm))):
        for r in range(first, last, BLK):
            rows = pl.ds(r, BLK)
            copies.append(pltpu.make_async_copy(src.at[rows], dst.at[rows], sem.at[n]))
    for c in copies:
        c.start()
    for c in copies:
        c.wait()


def writer_kernel(first, last, carried, ko_in, vo_in, *refs):
    write_rows(first, last, refs[0], refs[1], refs[carried], refs[carried + 1], refs[-1])


def solution(mesh):
    row_spec = P('dp', None)
    vec_spec = P(None)
    cache_spec = P('dp', 'tp', None, None)
    inv = np.power(np.float64(ROPE_BASE), -2.0 * np.arange(HALF, dtype=np.float64) / HEAD).astype(np.float32)
    inv_tab = np.broadcast_to(inv[:, None], (HALF, ROWS)).copy()
    bf16, f32 = jnp.bfloat16, jnp.float32
    sds = jax.ShapeDtypeStruct
    anyspec = pl.BlockSpec(memory_space=pl.ANY)
    vspec = pl.BlockSpec(memory_space=pltpu.VMEM)
    sspec = pl.BlockSpec(memory_space=pltpu.SMEM)
    dma = pltpu.SemaphoreType.DMA

    cache = (ROWS, KV, SEQ)
    main = pl.pallas_call(
        main_kernel,
        out_shape=(sds(cache, bf16), sds(cache, bf16), pltpu.VMEM(cache, bf16), pltpu.VMEM(cache, bf16),
                   pltpu.VMEM((HALF_ROWS, D), bf16), pltpu.VMEM((HALF_ROWS, D), f32), pltpu.VMEM((HALF_ROWS, D), bf16)),
        in_specs=[anyspec] * 14,
        out_specs=(anyspec,) * 2 + (vspec,) * 5,
        scratch_shapes=[
            pltpu.SMEM((ROWS,), jnp.int32), pltpu.VMEM((1, ROWS), jnp.int32), pltpu.VMEM((HALF, ROWS), f32),
            pltpu.VMEM((D,), f32), pltpu.VMEM((D,), f32), pltpu.VMEM((D,), f32), pltpu.VMEM((D,), f32),
            pltpu.VMEM((ROWS, D), bf16),
            pltpu.VMEM((3 * KV, D), bf16), pltpu.VMEM((WSLOTS, D, WCOLS), bf16),
            pltpu.VMEM((ROWS, D), bf16),
            pltpu.VMEM((ROWS, KV), f32), pltpu.VMEM((KV, ROWS), bf16), pltpu.VMEM((KV, ROWS), bf16),
            pltpu.VMEM((HALF_ROWS, D), f32), pltpu.VMEM((ROWS, KV), f32),
            pltpu.VMEM((BLK * 8, SEQ), f32), pltpu.VMEM((BLK * 8, SEQ), f32),
            dma((NBLK,)), dma((NBLK,)), dma((6 * KV // QROWS,)), dma((WSLOTS,)), dma, dma, dma, dma((7,)), dma((2, AHEAD)),
        ],
        compiler_params=pltpu.CompilerParams(vmem_limit_bytes=LIMIT),
        cost_estimate=pl.CostEstimate(flops=5 * 10**9, bytes_accessed=8 * 10**7, transcendentals=0),
        name='layer',
    )

    def writer(first, last, ko, vo, *carry):
        return pl.pallas_call(
            functools.partial(writer_kernel, first, last, len(carry)),
            out_shape=(sds(cache, bf16), sds(cache, bf16)) + tuple(pltpu.VMEM(c.shape, c.dtype) for c in carry),
            in_specs=[anyspec, anyspec] + [vspec] * len(carry),
            out_specs=(anyspec, anyspec) + (vspec,) * len(carry),
            scratch_shapes=[dma((2,))],
            input_output_aliases={n: n for n in range(2 + len(carry))},
            compiler_params=pltpu.CompilerParams(vmem_limit_bytes=LIMIT),
            cost_estimate=pl.CostEstimate(flops=(last - first) * 10**8, bytes_accessed=(last - first) * 4 * KV * SEQ, transcendentals=0),
            name='write%d' % first,
        )(ko, vo, *carry)

    def small(kernel, name):
        return pl.pallas_call(
            kernel, out_shape=pltpu.VMEM((HALF_ROWS, D), bf16), out_specs=vspec,
            compiler_params=pltpu.CompilerParams(vmem_limit_bytes=1 << 20), name=name)

    near_pairs = [(0, 1), (1, 0), (2, 3), (3, 2)]
    far_pairs = [(0, 2), (2, 0), (1, 3), (3, 1)]

    def device_step(x, ga, ba, gm, bm, w_qkv, w_out, w_up, w_down, k_cache, v_cache, positions):
        kt = jnp.swapaxes(k_cache, 2, 3).reshape(ROWS, KV, SEQ)
        vt = jnp.swapaxes(v_cache, 2, 3).reshape(ROWS, KV, SEQ)
        wq = jnp.transpose(w_qkv, (1, 2, 3, 0)).reshape(3 * KV, D)
        wo = w_out.reshape(KV, D)
        ko, vo, kbuf, vbuf, send, keep, xh = main(positions, positions.reshape(1, ROWS), jnp.asarray(inv_tab), ga, ba, gm, bm,
                                          x, wq, wo, w_up, w_down, kt, vt)
        near = lax.ppermute(send, 'tp', near_pairs)
        ko, vo, kbuf, vbuf, keep, xh = writer(CUTS[0], CUTS[1], ko, vo, kbuf, vbuf, keep, xh)
        mine = small(add_near, 'add_near')(keep, near)
        mine, ko, vo = lax.optimization_barrier((mine, ko, vo))
        far = lax.ppermute(mine, 'tp', far_pairs)
        ko, vo, kbuf, vbuf, xh = writer(CUTS[1], CUTS[2], ko, vo, kbuf, vbuf, xh)
        fin = small(add_far, 'add_far')(mine, far, xh)
        fin, ko, vo = lax.optimization_barrier((fin, ko, vo))
        other = lax.ppermute(fin, 'tp', near_pairs)
        ko, vo, kbuf, vbuf = writer(CUTS[2], ROWS, ko, vo, kbuf, vbuf)
        out = pl.pallas_call(
            assemble, out_shape=sds((ROWS, D), bf16), in_specs=[vspec] * 2, out_specs=anyspec,
            scratch_shapes=[dma((2,))], compiler_params=pltpu.CompilerParams(vmem_limit_bytes=1 << 20), name='assemble',
        )(fin, other)
        back = lambda c: jnp.swapaxes(c.reshape(ROWS, GROUPS, HEAD, SEQ), 2, 3)
        return out, back(ko), back(vo)

    return jax.shard_map(device_step, mesh=mesh, in_specs=(row_spec, vec_spec, vec_spec, vec_spec, vec_spec, P(None, 'tp', None, None), P('tp', None, None, None), P(None, 'tp'), P('tp', None), cache_spec, cache_spec, P('dp')), out_specs=(row_spec, cache_spec, cache_spec), check_vma=False)
```

```python
import functools
import numpy as np
import jax
import jax.numpy as jnp
from jax import lax
from jax.experimental import pallas as pl
from jax.experimental.pallas import tpu as pltpu
from jax.sharding import PartitionSpec as P

LN_EPS = 1e-5
ROPE_BASE = 10000.0
NEG_BIG = -1e30
MESH = pl.DeviceIdType.MESH

ROWS = 128
D = 2560
GROUPS = 8
HEAD = 80
HALF = 40
KV = GROUPS * HEAD
SEQ = 128
BLK = 8
NBLK = ROWS // BLK
WCOLS = 512
NW = D // WCOLS
WSLOTS = 3
QROWS = 960
AHEAD = 4
OCOLS = 1280
OROWS = 8
HALF_ROWS = ROWS // 2
CUTS = (AHEAD * OROWS, 40, 120)
LIMIT = 22784 << 10


def main_kernel(pos_hbm, pos_row_hbm, inv_hbm, ga_hbm, ba_hbm, gm_hbm, bm_hbm, x_hbm, wq_hbm, wo_hbm, wu_hbm, wd_hbm, k_hbm, v_hbm,
                ko_hbm, vo_hbm, kbuf, vbuf, send_ref, keep_ref, xh_ref,
                pos_smem, pos_row, inv_freq, ga, ba, gm, bm, x_ref, wqbuf, wbuf, ain, qrows, kt_sc, vt_sc, acc, ctx, s_sc, p_sc,
                ksem, vsem, wqsem, wsem, wosem, xsem, xhsem, smsem, outsem):
    f32, bf16 = jnp.float32, jnp.bfloat16
    h_sc, min_ = ain, x_ref

    def wq_copy(n):
        rows = pl.ds(n * (QROWS // 2), QROWS // 2)
        return pltpu.make_async_copy(wq_hbm.at[rows], wqbuf.at[rows], wqsem.at[n])

    def wo_copy():
        return pltpu.make_async_copy(wo_hbm, wqbuf.at[pl.ds(0, KV)], wosem)

    def k_copy(i):
        rows = pl.ds(i * BLK, BLK)
        return pltpu.make_async_copy(k_hbm.at[rows], kbuf.at[rows], ksem.at[i])

    def v_copy(i):
        rows = pl.ds(i * BLK, BLK)
        return pltpu.make_async_copy(v_hbm.at[rows], vbuf.at[rows], vsem.at[i])

    def kv_start(i):
        k_copy(i).start()
        v_copy(i).start()

    def w_copy(hbm, c, n):
        cols = pl.ds(pl.multiple_of(c * WCOLS, WCOLS), WCOLS)
        slot = lax.rem(n, WSLOTS)
        return pltpu.make_async_copy(hbm.at[:, cols], wbuf.at[slot], wsem.at[slot])

    x_copy = pltpu.make_async_copy(x_hbm, x_ref, xsem)
    small = [pltpu.make_async_copy(src, dst, smsem.at[n]) for n, (src, dst) in enumerate((
        (pos_hbm, pos_smem), (pos_row_hbm, pos_row), (inv_hbm, inv_freq),
        (ga_hbm, ga), (ba_hbm, ba), (gm_hbm, gm), (bm_hbm, bm)))]
    x_copy.start()
    for c in small:
        c.start()
    wq_copy(0).start()
    for c in small:
        c.wait()
    x_copy.wait()
    for n in range(1, 4):
        wq_copy(n).start()
    core = lax.rem(lax.axis_index('tp'), 2)
    mine_rows = pl.ds(pl.multiple_of(core * HALF_ROWS, HALF_ROWS), HALF_ROWS)
    xh_copy = pltpu.make_async_copy(x_hbm.at[mine_rows], xh_ref, xhsem)
    xh_copy.start()

    gav, bav, gmv, bmv = [r[...].reshape(1, D) for r in (ga, ba, gm, bm)]
    for r in range(0, ROWS, 16):
        rows = slice(r, r + 16)
        xf = x_ref[rows, :].astype(f32)
        mean = jnp.mean(xf, axis=-1, keepdims=True)
        cen = xf - mean
        var = jnp.mean(cen * cen, axis=-1, keepdims=True)
        nrm = cen * lax.rsqrt(var + LN_EPS)
        ain[rows, :] = (nrm * gav + bav).astype(bf16)
        min_[rows, :] = (nrm * gmv + bmv).astype(bf16)

    angles = inv_freq[...] * pos_row[...].astype(f32)
    cos_t = jnp.cos(angles)
    sin_t = jnp.sin(angles)

    def rotate(u):
        lo, hi = u[:HALF], u[HALF:]
        return jnp.concatenate([lo * cos_t - hi * sin_t, hi * cos_t + lo * sin_t], axis=0).astype(bf16)

    queries = []
    for n in range(3 * KV // QROWS):
        wq_copy(2 * n).wait()
        wq_copy(2 * n + 1).wait()
        if n == 0:
            kv_start(0)
            w_copy(wu_hbm, 0, 0).start()
            kv_start(1)
        else:
            w_copy(wu_hbm, 1, 1).start()
            kv_start(2)
            w_copy(wu_hbm, 2, 2).start()
        y = jnp.concatenate([
            lax.dot_general(wqbuf[r:r + QROWS // 2, :], ain[...], (((1,), (1,)), ((), ())), preferred_element_type=f32)
            for r in (n * QROWS, n * QROWS + QROWS // 2)], axis=0)
        y = y.astype(bf16).astype(f32)
        for m in range(QROWS // (3 * HEAD)):
            g = n * (QROWS // (3 * HEAD)) + m
            yg = y[m * 3 * HEAD:(m + 1) * 3 * HEAD]
            feat = slice(g * HEAD, (g + 1) * HEAD)
            queries.append(rotate(yg[:HEAD]).astype(f32))
            kt_sc[feat, :] = rotate(yg[HEAD:2 * HEAD])
            vt_sc[feat, :] = yg[2 * HEAD:].astype(bf16)
    for i in range(3, AHEAD):
        kv_start(i)
    qall = jnp.concatenate(queries, axis=0)
    for c in range(KV // 128):
        qrows[:, c * 128:(c + 1) * 128] = qall[c * 128:(c + 1) * 128, :].T

    lane8 = lax.broadcasted_iota(jnp.int32, (8, KV), 1)
    sub8 = lax.broadcasted_iota(jnp.int32, (8, KV), 0)
    own8 = (lane8 >= sub8 * HEAD) & (lane8 < sub8 * HEAD + HEAD)
    s_lane = lax.broadcasted_iota(jnp.int32, (8, SEQ), 1)
    c_lane = lax.broadcasted_iota(jnp.int16, (KV, SEQ), 1)
    top16 = lax.broadcasted_iota(jnp.int32, (16, SEQ), 0) < 8
    sel = (lax.broadcasted_iota(jnp.int32, (BLK, BLK * 8), 1) // 8
           == lax.broadcasted_iota(jnp.int32, (BLK, BLK * 8), 0)).astype(f32).astype(bf16)

    def arrive(i):
        k_copy(i).wait()
        v_copy(i).wait()

    def scores(i):
        base = pl.multiple_of(i * BLK, BLK)
        for j in range(0, BLK, 2):
            qs, ks = [], []
            for b in (base + j, base + j + 1):
                t = pos_smem[b]
                shift = lax.rem(t - b + SEQ, SEQ)
                hit = c_lane == t.astype(jnp.int16)
                kn = jnp.where(hit, pltpu.roll(kt_sc[...], shift, 1), kbuf[b])
                kbuf[b] = kn
                ks.append(kn)
                vbuf[b] = jnp.where(hit, pltpu.roll(vt_sc[...], shift, 1), vbuf[b])
                row = jnp.broadcast_to(qrows[pl.ds(b, 1), :], (8, KV))
                qs.append(jnp.where(own8, row, 0.0))
            s2 = jnp.dot(jnp.concatenate(qs, axis=0).astype(bf16), jnp.concatenate(ks, axis=1), preferred_element_type=f32)
            s_sc[j * 8:j * 8 + 8, :] = s2[:8, :SEQ]
            s_sc[j * 8 + 8:j * 8 + 16, :] = s2[8:, SEQ:]

    def soften(i):
        for j in range(BLK):
            s = s_sc[j * 8:j * 8 + 8, :] * (HEAD ** -0.5)
            s = jnp.where(s_lane <= pos_smem[i * BLK + j], s, NEG_BIG)
            e = jnp.exp(s - jnp.max(s, axis=-1, keepdims=True))
            p_sc[j * 8:j * 8 + 8, :] = e / jnp.sum(e, axis=-1, keepdims=True)

    def mix(i):
        base = pl.multiple_of(i * BLK, BLK)
        picked = []
        for j in range(0, BLK, 2):
            p = p_sc[j * 8:j * 8 + 16, :]
            pbd = jnp.concatenate([jnp.where(top16, p, 0.0), jnp.where(top16, 0.0, p)], axis=1).astype(bf16)
            vv = jnp.concatenate([vbuf[base + j], vbuf[base + j + 1]], axis=1)
            c2 = lax.dot_general(pbd, vv, (((1,), (1,)), ((), ())), preferred_element_type=f32)
            picked.append(jnp.where(own8, c2[:8], 0.0))
            picked.append(jnp.where(own8, c2[8:], 0.0))
        stack = jnp.concatenate(picked, axis=0).astype(bf16)
        ctx[pl.ds(base, BLK), :] = jnp.dot(sel, stack, preferred_element_type=f32)

    def attend(i):
        mix(jnp.maximum(i - 2, 0))
        soften(jnp.maximum(i - 1, 0))
        scores(i)

    def split(y):
        low, high = y[:HALF_ROWS], y[HALF_ROWS:]
        return jnp.where(core == 0, low, high), jnp.where(core == 0, high, low)

    def up_dot(c):
        y = jnp.dot(min_[...], wbuf[lax.rem(c, WSLOTS)], preferred_element_type=f32)
        cols = pl.ds(pl.multiple_of(c * WCOLS, WCOLS), WCOLS)
        h_sc[:, cols] = (0.5 * y * (1.0 + lax.erf(y * (0.5 ** 0.5)))).astype(bf16)

    def down_dot(c, n):
        cols = pl.ds(pl.multiple_of(c * WCOLS, WCOLS), WCOLS)
        mine, near = split(jnp.dot(h_sc[...], wbuf[lax.rem(n, WSLOTS)], preferred_element_type=f32))
        keep_ref[:, cols] = mine
        acc[:, cols] = near

    def out_copies(j):
        rows = pl.ds(j * OROWS, OROWS)
        return [pltpu.make_async_copy(src.at[rows], dst.at[rows], outsem.at[n, j])
                for n, (src, dst) in enumerate(((kbuf, ko_hbm), (vbuf, vo_hbm)))]

    s_sc[...] = jnp.zeros_like(s_sc)
    p_sc[...] = jnp.zeros_like(p_sc)

    def up_body(next_hbm, back, c, _):
        w_copy(wu_hbm, c, c).wait()
        arrive(c)
        up_dot(c)
        attend(c)
        w_copy(next_hbm, c + WSLOTS - back, c + WSLOTS).start()
        kv_start(c + AHEAD)
        return 0

    def down_body(more, c, _):
        n = c + NW
        w_copy(wd_hbm, c, n).wait()
        arrive(n)
        down_dot(c, n)
        attend(n)
        if more:
            w_copy(wd_hbm, c + WSLOTS, n + WSLOTS).start()
        kv_start(n + AHEAD)
        return 0

    def rest_body(more, i, _):
        arrive(i)
        if more:
            kv_start(i + AHEAD)
        else:
            for c in out_copies(i - (NBLK - AHEAD)):
                c.start()
        attend(i)
        return 0

    lax.fori_loop(0, NW - WSLOTS, functools.partial(up_body, wu_hbm, 0), 0)
    lax.fori_loop(NW - WSLOTS, NW, functools.partial(up_body, wd_hbm, NW), 0)
    lax.fori_loop(0, NW - WSLOTS, functools.partial(down_body, True), 0)
    lax.fori_loop(NW - WSLOTS, NW, functools.partial(down_body, False), 0)
    wo_copy().start()
    lax.fori_loop(2 * NW, NBLK - AHEAD, functools.partial(rest_body, True), 0)
    lax.fori_loop(NBLK - AHEAD, NBLK, functools.partial(rest_body, False), 0)
    wo_copy().wait()
    mix(NBLK - 2)
    soften(NBLK - 1)
    mix(NBLK - 1)

    cb = ctx[...].astype(bf16)
    for c in range(0, D, OCOLS):
        cols = slice(c, c + OCOLS)
        mine, near = split(jnp.dot(cb, wqbuf[0:KV, cols], preferred_element_type=f32))
        keep_ref[:, cols] += mine
        send_ref[:, cols] = (acc[:, cols] + near).astype(bf16)
    xh_copy.wait()
    for j in range(AHEAD):
        for c in out_copies(j):
            c.wait()


def add_near(keep, near, mine):
    mine[...] = (keep[...] + near[...].astype(jnp.float32)).astype(jnp.bfloat16)


def add_far(mine, far, xh, fin):
    f32 = jnp.float32
    fin[...] = (mine[...].astype(f32) + far[...].astype(f32) + xh[...].astype(f32)).astype(jnp.bfloat16)


def assemble(fin, other, out_hbm, sem):
    core = lax.rem(lax.axis_index('tp'), 2)
    copies = []
    for n, (src, place) in enumerate(((fin, core), (other, 1 - core))):
        rows = pl.ds(pl.multiple_of(place * HALF_ROWS, HALF_ROWS), HALF_ROWS)
        copies.append(pltpu.make_async_copy(src, out_hbm.at[rows], sem.at[n]))
    for c in copies:
        c.start()
    for c in copies:
        c.wait()


def write_rows(first, last, kbuf, vbuf, ko_hbm, vo_hbm, sem):
    copies = []
    for n, (src, dst) in enumerate(((kbuf, ko_hbm), (vbuf, vo_hbm))):
        for r in range(first, last, BLK):
            rows = pl.ds(r, BLK)
            copies.append(pltpu.make_async_copy(src.at[rows], dst.at[rows], sem.at[n]))
    for c in copies:
        c.start()
    for c in copies:
        c.wait()


def writer_kernel(first, last, carried, ko_in, vo_in, *refs):
    write_rows(first, last, refs[0], refs[1], refs[carried], refs[carried + 1], refs[-1])


def solution(mesh):
    row_spec = P('dp', None)
    vec_spec = P(None)
    cache_spec = P('dp', 'tp', None, None)
    inv = np.power(np.float64(ROPE_BASE), -2.0 * np.arange(HALF, dtype=np.float64) / HEAD).astype(np.float32)
    inv_tab = np.broadcast_to(inv[:, None], (HALF, ROWS)).copy()
    bf16, f32 = jnp.bfloat16, jnp.float32
    sds = jax.ShapeDtypeStruct
    anyspec = pl.BlockSpec(memory_space=pl.ANY)
    vspec = pl.BlockSpec(memory_space=pltpu.VMEM)
    sspec = pl.BlockSpec(memory_space=pltpu.SMEM)
    dma = pltpu.SemaphoreType.DMA

    cache = (ROWS, KV, SEQ)
    main = pl.pallas_call(
        main_kernel,
        out_shape=(sds(cache, bf16), sds(cache, bf16), pltpu.VMEM(cache, bf16), pltpu.VMEM(cache, bf16),
                   pltpu.VMEM((HALF_ROWS, D), bf16), pltpu.VMEM((HALF_ROWS, D), f32), pltpu.VMEM((HALF_ROWS, D), bf16)),
        in_specs=[anyspec] * 14,
        out_specs=(anyspec,) * 2 + (vspec,) * 5,
        scratch_shapes=[
            pltpu.SMEM((ROWS,), jnp.int32), pltpu.VMEM((1, ROWS), jnp.int32), pltpu.VMEM((HALF, ROWS), f32),
            pltpu.VMEM((D,), f32), pltpu.VMEM((D,), f32), pltpu.VMEM((D,), f32), pltpu.VMEM((D,), f32),
            pltpu.VMEM((ROWS, D), bf16),
            pltpu.VMEM((3 * KV, D), bf16), pltpu.VMEM((WSLOTS, D, WCOLS), bf16),
            pltpu.VMEM((ROWS, D), bf16),
            pltpu.VMEM((ROWS, KV), f32), pltpu.VMEM((KV, ROWS), bf16), pltpu.VMEM((KV, ROWS), bf16),
            pltpu.VMEM((HALF_ROWS, D), f32), pltpu.VMEM((ROWS, KV), f32),
            pltpu.VMEM((BLK * 8, SEQ), f32), pltpu.VMEM((BLK * 8, SEQ), f32),
            dma((NBLK,)), dma((NBLK,)), dma((6 * KV // QROWS,)), dma((WSLOTS,)), dma, dma, dma, dma((7,)), dma((2, AHEAD)),
        ],
        compiler_params=pltpu.CompilerParams(vmem_limit_bytes=LIMIT),
        cost_estimate=pl.CostEstimate(flops=5 * 10**9, bytes_accessed=8 * 10**7, transcendentals=0),
        name='layer',
    )

    def writer(first, last, ko, vo, *carry):
        return pl.pallas_call(
            functools.partial(writer_kernel, first, last, len(carry)),
            out_shape=(sds(cache, bf16), sds(cache, bf16)) + tuple(pltpu.VMEM(c.shape, c.dtype) for c in carry),
            in_specs=[anyspec, anyspec] + [vspec] * len(carry),
            out_specs=(anyspec, anyspec) + (vspec,) * len(carry),
            scratch_shapes=[dma((2,))],
            input_output_aliases={n: n for n in range(2 + len(carry))},
            compiler_params=pltpu.CompilerParams(vmem_limit_bytes=LIMIT),
            cost_estimate=pl.CostEstimate(flops=(last - first) * 10**8, bytes_accessed=(last - first) * 4 * KV * SEQ, transcendentals=0),
            name='write%d' % first,
        )(ko, vo, *carry)

    def small(kernel, name):
        return pl.pallas_call(
            kernel, out_shape=pltpu.VMEM((HALF_ROWS, D), bf16), out_specs=vspec,
            compiler_params=pltpu.CompilerParams(vmem_limit_bytes=1 << 20), name=name)

    near_pairs = [(0, 1), (1, 0), (2, 3), (3, 2)]
    far_pairs = [(0, 2), (2, 0), (1, 3), (3, 1)]

    def device_step(x, ga, ba, gm, bm, w_qkv, w_out, w_up, w_down, k_cache, v_cache, positions):
        kt = jnp.swapaxes(k_cache, 2, 3).reshape(ROWS, KV, SEQ)
        vt = jnp.swapaxes(v_cache, 2, 3).reshape(ROWS, KV, SEQ)
        wq = jnp.transpose(w_qkv, (1, 2, 3, 0)).reshape(3 * KV, D)
        wo = w_out.reshape(KV, D)
        ko, vo, kbuf, vbuf, send, keep, xh = main(positions, positions.reshape(1, ROWS), jnp.asarray(inv_tab), ga, ba, gm, bm,
                                          x, wq, wo, w_up, w_down, kt, vt)
        near = lax.ppermute(send, 'tp', near_pairs)
        ko, vo, kbuf, vbuf, keep, xh = writer(CUTS[0], CUTS[1], ko, vo, kbuf, vbuf, keep, xh)
        mine = small(add_near, 'add_near')(keep, near)
        mine, ko, vo = lax.optimization_barrier((mine, ko, vo))
        far = lax.ppermute(mine, 'tp', far_pairs)
        ko, vo, kbuf, vbuf, xh = writer(CUTS[1], CUTS[2], ko, vo, kbuf, vbuf, xh)
        fin = small(add_far, 'add_far')(mine, far, xh)
        fin, ko, vo = lax.optimization_barrier((fin, ko, vo))
        other = lax.ppermute(fin, 'tp', near_pairs)
        ko, vo, kbuf, vbuf = writer(CUTS[2], ROWS, ko, vo, kbuf, vbuf)
        out = pl.pallas_call(
            assemble, out_shape=sds((ROWS, D), bf16), in_specs=[vspec] * 2, out_specs=anyspec,
            scratch_shapes=[dma((2,))], compiler_params=pltpu.CompilerParams(vmem_limit_bytes=1 << 20), name='assemble',
        )(fin, other)
        back = lambda c: jnp.swapaxes(c.reshape(ROWS, GROUPS, HEAD, SEQ), 2, 3)
        return out, back(ko), back(vo)

    return jax.shard_map(device_step, mesh=mesh, in_specs=(row_spec, vec_spec, vec_spec, vec_spec, vec_spec, P(None, 'tp', None, None), P('tp', None, None, None), P(None, 'tp'), P('tp', None), cache_spec, cache_spec, P('dp')), out_specs=(row_spec, cache_spec, cache_spec), check_vma=False)
```
